32 devices in a mesh: groups: 2 (over y), ep: 8 (over z, core), tp: 2 (over x).
Axes of the slice: x: 2, y: 2, z: 4, core: 2. Of those that a mesh axis runs over, the one named last changes fastest.
Arguments:
- hidden: bfloat16 [1024, 2880], P(('groups', 'ep')), parts along dimension 0, may hold values from -6 to 6
- route_experts: int32 [1024, 4], P(('groups', 'ep')), parts along dimension 0, may hold values from 0 to 7, all different within a row; in each aligned block of 64 rows (0 to 63, 64 to 127, ...) at most 64 rows name the same one
- route_weight: float32 [1024, 4], P(('groups', 'ep')), parts along dimension 0, may hold values from 0.1 to 0.6
- norm_gain: bfloat16 [2880], replicated, may hold values from 0.099609375 to 1.8984375
- gate_up_codes: int32 [8, 360, 5120], P('ep', None, 'tp'), may hold values from -2147483648 to 2147483646
- gate_up_scales: bfloat16 [8, 90, 5120], P('ep', None, 'tp'), as said below
- gate_up_bias: bfloat16 [8, 5120], P('ep', 'tp'), may hold values from -3 to 3
- down_codes: int32 [8, 2560, 360], P('ep', 'tp'), may hold values from -2147483648 to 2147483646
- down_scales: bfloat16 [8, 80, 2880], P('ep', 'tp'), as said below
- down_bias: bfloat16 [8, 2880], P('ep', 'tp'), may hold values from -3 to 3
Outputs:
- layer_out: bfloat16 [1024, 2880], P(('groups', 'ep'), 'tp'), parts along dimension 0
The draws below stay inside these ranges and needn't reach their ends.
There are 2 independent parts, one for each index of `groups`. The reference program is written for one: setup_inputs(seed, part) draws one part's arguments, and reference() takes and returns one part's arrays. A program takes and returns all parts, laid end to end along the dimension named above; an argument that names none is the same for every part. Nothing has to cross between parts.
Inputs may be any that keep to these rules, and one draw needn't show every extreme that they name: `route_experts`: each row names 4 different experts. In each aligned block of 64 rows no expert is named by more than 64 rows, and in some blocks one expert is named by exactly 64 rows. `gate_up_scales`: every scale is a power of two. `down_scales`: every scale is a power of two.
All inputs are finite; a program needn't handle non-finite values.
Results may differ from the reference program's by a relative error of at most 0.013.
Values may be sent and summed in bfloat16 or wider, within the bound.
A program may use at most 128 MiB of HBM per device.

```python
import math
import jax
import jax.numpy as jnp
import numpy as np
from jax import lax

D = 2880
TOP = 4
FF = 2560
TOK_EP = 64
EXPERTS = 8
TOKENS = 512
CAP = 64
N_EP = 8
N_TP = 2


def draw_gate_up_scales(key, part):
    centre = int(math.floor(math.log2(0.5 / math.sqrt(D))))
    powers = jax.random.randint(jax.random.fold_in(key, 11), (EXPERTS, D // 32, 2 * FF), centre - 1, centre + 2)
    return jnp.exp2(powers.astype(jnp.float32)).astype(jnp.bfloat16)


def draw_down_scales(key, part):
    centre = int(math.floor(math.log2(0.5 / math.sqrt(FF))))
    powers = jax.random.randint(jax.random.fold_in(key, 23), (EXPERTS, FF // 32, D), centre - 1, centre + 2)
    return jnp.exp2(powers.astype(jnp.float32)).astype(jnp.bfloat16)


def place_ends(entries, stream_key, smallest, largest):
    extent = entries.shape
    index_at = [jax.random.randint(jax.random.fold_in(stream_key, axis), (), 0, extent[axis]) for axis in range(len(extent))]
    entries = entries.at[tuple(index_at)].set(smallest)
    longest = extent.index(max(extent))
    index_at[longest] = (index_at[longest] + 1) % extent[longest]
    return entries.at[tuple(index_at)].set(largest)


def shard_levels(own_key, extent, cuts, low, high):
    def one(axis_at, blocks):
        heights = jax.random.uniform(jax.random.fold_in(jax.random.fold_in(own_key, 6), axis_at), (blocks,), jnp.float32, low / len(cuts), high / len(cuts))
        return jnp.repeat(jnp.exp(heights), extent[axis_at] // blocks).reshape((-1,) + (1,) * (len(extent) - axis_at - 1))

    level = one(*cuts[0])
    for cut in cuts[1:]:
        level = level * one(*cut)
    return level


def shared_out(rng, own, number, rows, amount, top, reach, slope):
    ranking = jax.random.permutation(rng, amount)
    crowded, common = load_shares(amount, rows * top, reach, slope, True), load_shares(amount, rows * top, reach, slope, False)
    places = jnp.arange(amount)

    def named(lengths, offset_by):
        used = int((lengths > 0).sum())
        fixed = max(1, used // 4)
        moved = fixed + (places - fixed + offset_by * (used - fixed)) % max(1, amount - fixed)
        return jnp.zeros((amount,), jnp.int32).at[ranking[jnp.where(places < fixed, places, moved)]].set(jnp.asarray(lengths, jnp.int32))

    lengths = jnp.where(number % 4 == 0, named(crowded, number // 4), named(common, number - number // 4 - 1))
    mixed = jax.random.permutation(jax.random.fold_in(own, 3), amount)
    giver, taker = mixed[0:amount // 2 * 2:2], mixed[1:amount // 2 * 2:2]
    margin = jnp.minimum(lengths[giver] - 1, reach - lengths[taker]) // 2
    margin = jnp.where((giver == ranking[0]) | (taker == ranking[0]) | (lengths[taker] == 0), 0, jnp.maximum(margin, 0))
    moved = jax.random.randint(jax.random.fold_in(own, 4), (amount // 2,), 0, 1 << 20) % (margin + 1)
    lengths = lengths.at[giver].add(-moved).at[taker].add(moved)
    items = jnp.searchsorted(jnp.cumsum(lengths), jnp.arange(rows * top), side="right").astype(jnp.int32)
    grid = items.reshape(top, rows).T
    grid = grid[jax.random.permutation(jax.random.fold_in(own, 1), rows)]
    offset_by = jax.random.randint(jax.random.fold_in(own, 2), (rows, 1), 0, top)
    return jnp.take_along_axis(grid, (jnp.arange(top)[None, :] + offset_by) % top, axis=1)


def load_shares(number_of, total, reach, skew, full):
    portions = [(1 << 20) // math.isqrt(standing ** skew) + 1 for standing in range(1, number_of + 1)]
    largest = reach if full else min(reach, max(-(-total // number_of), total * portions[0] // sum(portions)))
    least = 1 if total - largest >= number_of - 1 else 0
    holding, surplus = [largest] + [least] * (number_of - 1), total - largest - least * (number_of - 1)
    while surplus > 0:
        free = [i for i in range(1, number_of) if holding[i] < largest] or [i for i in range(1, number_of) if holding[i] < reach]
        whole, budget = sum([portions[i] for i in free]), surplus
        for i in free:
            extra = min(reach - holding[i], max(1, budget * portions[i] // whole), surplus)
            holding[i] = holding[i] + extra
            surplus = surplus - extra
    return np.array(holding)


def bell_draw(rng, extent, spread, reach, shards=(), held_as=jnp.bfloat16):
    gain = shard_levels(rng, extent, shards, -0.22, 0.18) if shards else 1.0
    entries = jax.random.normal(rng, extent, jnp.float32) * spread * gain
    return jnp.minimum(jnp.maximum(entries, -reach), reach).astype(held_as)


def setup_inputs(seed: int = 0, part: int = 0) -> dict:
    key_of = jax.random.split(jax.random.key(seed), 11)
    part_splits = jax.random.split(jax.random.fold_in(key_of[10], part), 11)
    hidden = bell_draw(part_splits[0], (TOKENS, D), 1.0, 6.0, ((0, 8),))
    route_experts_keys = jax.random.split(jax.random.fold_in(part_splits[1], 1), TOKENS // TOK_EP)
    route_experts_turns = jax.random.permutation(jax.random.fold_in(part_splits[1], 3), TOKENS // TOK_EP)
    route_experts = jax.vmap(lambda own, number: shared_out(jax.random.fold_in(part_splits[1], 2), own, number, TOK_EP, EXPERTS, TOP, CAP, 2))(route_experts_keys, route_experts_turns).reshape((TOKENS, TOP))
    route_weight = jnp.clip(0.1 + 0.5 * jax.random.uniform(part_splits[2], (TOKENS, TOP), jnp.float32) ** shard_levels(part_splits[2], (TOKENS, TOP), ((0, 8),), -0.2, 0.2), 0.1, 0.6)
    norm_gain = jnp.clip(1.0 + 0.18 * jax.random.normal(key_of[3], (D,), jnp.float32), 0.099609375, 1.8984375).astype(jnp.bfloat16)
    gate_up_codes = place_ends(jax.random.randint(key_of[4], (EXPERTS, D // 8, 2 * FF), -2147483648, 2147483647), jax.random.fold_in(key_of[4], 1), -2147483648, 2147483646).astype(jnp.int32)
    gate_up_scales = draw_gate_up_scales(jax.random.fold_in(key_of[10], 71), part)
    gate_up_bias = bell_draw(key_of[6], (EXPERTS, 2 * FF), 0.5, 3.0, ((0, 8), (1, 2)))
    down_codes = place_ends(jax.random.randint(key_of[7], (EXPERTS, FF, D // 8), -2147483648, 2147483647), jax.random.fold_in(key_of[7], 1), -2147483648, 2147483646).astype(jnp.int32)
    down_scales = draw_down_scales(jax.random.fold_in(key_of[10], 71), part)
    down_bias = bell_draw(key_of[9], (EXPERTS, D), 0.5, 3.0, ((0, 8), (1, 2)))
    return {"hidden": hidden, "route_experts": route_experts, "route_weight": route_weight, "norm_gain": norm_gain, "gate_up_codes": gate_up_codes, "gate_up_scales": gate_up_scales, "gate_up_bias": gate_up_bias, "down_codes": down_codes, "down_scales": down_scales, "down_bias": down_bias}


def decode_nibble(nibble):
    magnit = nibble & 7
    exponent = jnp.maximum(jnp.right_shift(magnit, 1) - 1, 0)
    doubled = jnp.where(magnit < 2, magnit, jnp.left_shift(2 + (magnit & 1), exponent))
    signed_val = doubled.astype(jnp.float32) * 0.5
    return jnp.where(nibble >= 8, -signed_val, signed_val)

def unpack_weights(packed, scaling):
    row_count = packed.shape[0]
    shifts = jnp.arange(8, dtype=jnp.int32) * 4
    nibble = jnp.right_shift(packed[:, :, None], shifts[None, None, :]) & 15
    nibble = nibble.reshape(row_count, packed.shape[1] * 8)
    signed_val = decode_nibble(nibble)
    signed_val = signed_val.reshape(row_count // 32, 32, -1) * scaling.astype(jnp.float32)[:, None, :]
    return signed_val.reshape(row_count, -1).astype(jnp.bfloat16)

def unpack_rows(packed, scaling):
    row_count = packed.shape[0] * 8
    shifts = jnp.arange(8, dtype=jnp.int32) * 4
    nibble = jnp.right_shift(packed[:, None, :], shifts[None, :, None]) & 15
    nibble = nibble.reshape(row_count, packed.shape[1])
    signed_val = decode_nibble(nibble)
    signed_val = signed_val.reshape(row_count // 32, 32, -1) * scaling.astype(jnp.float32)[:, None, :]
    return signed_val.reshape(row_count, -1).astype(jnp.bfloat16)

def rms_normed(hidden, norm_gain):
    widened = hidden.astype(jnp.float32)
    mean_square = lax.optimization_barrier(jnp.mean(widened * widened, axis=-1, keepdims=True))
    scaled = widened * lax.rsqrt(mean_square + 1e-05) * norm_gain.astype(jnp.float32)
    return scaled.astype(jnp.bfloat16)

def slot_numbers(routes):
    block_count, row_count, top_count = routes.shape
    flat_routes = routes.reshape(block_count, row_count * top_count)
    onehot = (flat_routes[:, :, None] == jnp.arange(EXPERTS, dtype=jnp.int32)[None, None, :]).astype(jnp.int32)
    before = jnp.cumsum(onehot, axis=1) - onehot
    slot_of = lax.optimization_barrier(jnp.sum(before * onehot, axis=2))
    return slot_of.reshape(block_count, row_count, top_count)

def expert_rows(normed_rows, gate_codes, gate_scales, gate_bias, lower_codes, lower_scales, lower_bias):
    gate_up_weight = unpack_rows(gate_codes, gate_scales)
    down_weight = unpack_weights(lower_codes, lower_scales)
    projected = jnp.dot(normed_rows, gate_up_weight, preferred_element_type=jnp.float32) + gate_bias.astype(jnp.float32)
    gate_part = jnp.minimum(projected[:, 0::2], 7.0)
    upward = jnp.clip(projected[:, 1::2], -7.0, 7.0)
    activated = (gate_part * jax.nn.sigmoid(1.702 * gate_part) * (upward + 1.0)).astype(jnp.bfloat16)
    quarter = FF // N_TP
    summed = jnp.zeros((normed_rows.shape[0], D), jnp.float32)
    for tp_part in range(N_TP):
        partial_value = jnp.dot(activated[:, tp_part * quarter:(tp_part + 1) * quarter], down_weight[tp_part * quarter:(tp_part + 1) * quarter], preferred_element_type=jnp.float32).astype(jnp.bfloat16)
        summed = summed + partial_value.astype(jnp.float32)
    return (summed + lower_bias.astype(jnp.float32)).astype(jnp.bfloat16)

def reference(hidden, route_experts, route_weight, norm_gain, gate_up_codes, gate_up_scales, gate_up_bias, down_codes, down_scales, down_bias):
    normed = rms_normed(hidden, norm_gain)
    routes = route_experts.reshape(N_EP, TOK_EP, TOP)
    slot_of = slot_numbers(routes)
    token_ids = jnp.broadcast_to(jnp.arange(TOKENS, dtype=jnp.int32).reshape(N_EP, TOK_EP, 1), routes.shape)
    block_ids = jnp.broadcast_to(jnp.arange(N_EP, dtype=jnp.int32).reshape(N_EP, 1, 1), routes.shape)
    slot_table = jnp.zeros((EXPERTS, N_EP, CAP), jnp.int32).at[routes, block_ids, slot_of].set(token_ids)

    def one_expert(expert):
        picked = normed[slot_table[expert].reshape(-1)]
        return expert_rows(picked, gate_up_codes[expert], gate_up_scales[expert], gate_up_bias[expert], down_codes[expert], down_scales[expert], down_bias[expert])
    outputs = lax.map(one_expert, jnp.arange(EXPERTS, dtype=jnp.int32)).reshape(EXPERTS, N_EP, CAP, D)
    weights = route_weight.reshape(N_EP, TOK_EP, TOP)
    running = hidden.astype(jnp.float32).reshape(N_EP, TOK_EP, D)
    for position in range(TOP):
        fetched = outputs[routes[:, :, position], block_ids[:, :, position], slot_of[:, :, position]]
        running = running + weights[:, :, position][:, :, None] * fetched.astype(jnp.float32)
    return running.reshape(TOKENS, D).astype(jnp.bfloat16)
```

```python
import functools

import jax
import jax.numpy as jnp
from jax import lax
from jax.experimental import pallas as pl
from jax.experimental.pallas import tpu as pltpu
from jax.sharding import PartitionSpec as P

MAGNITUDES = 0xC8643210 - (1 << 32)
SPARE = 64


def decode_nibble(nibble):
    magnit = nibble & 7
    exponent = jnp.maximum(jnp.right_shift(magnit, 1) - 1, 0)
    doubled = jnp.where(magnit < 2, magnit, jnp.left_shift(2 + (magnit & 1), exponent))
    signed_val = doubled.astype(jnp.float32) * 0.5
    return jnp.where(nibble >= 8, -signed_val, signed_val)


def unpack_weights(packed, scaling):
    row_count = packed.shape[0]
    shifts = jnp.arange(8, dtype=jnp.int32) * 4
    nibble = jnp.right_shift(packed[:, :, None], shifts[None, None, :]) & 15
    nibble = nibble.reshape(row_count, packed.shape[1] * 8)
    signed_val = decode_nibble(nibble)
    signed_val = (
        signed_val.reshape(row_count // 32, 32, -1) * scaling.astype(jnp.float32)[:, None, :]
    )
    return signed_val.reshape(row_count, -1).astype(jnp.bfloat16)


def unpack_rows(packed, scaling):
    row_count = packed.shape[0] * 8
    shifts = jnp.arange(8, dtype=jnp.int32) * 4
    nibble = jnp.right_shift(packed[:, None, :], shifts[None, :, None]) & 15
    nibble = nibble.reshape(row_count, packed.shape[1])
    signed_val = decode_nibble(nibble)
    signed_val = (
        signed_val.reshape(row_count // 32, 32, -1) * scaling.astype(jnp.float32)[:, None, :]
    )
    return signed_val.reshape(row_count, -1).astype(jnp.bfloat16)


def rms_normed(hidden, norm_gain):
    widened = hidden.astype(jnp.float32)
    mean_square = jnp.mean(widened * widened, axis=-1, keepdims=True)
    scaled = widened * lax.rsqrt(mean_square + 1e-05) * norm_gain.astype(jnp.float32)
    return scaled.astype(jnp.bfloat16)


def shards(
    hidden,
    route_experts,
    route_weight,
    norm_gain,
    gate_up_codes,
    gate_up_scales,
    gate_up_bias,
    down_codes,
    down_scales,
    down_bias,
):
    ep_count = lax.axis_size("ep")
    tp_count = lax.axis_size("tp")
    tp_rank = lax.axis_index("tp")
    tok_count, model_width = hidden.shape
    top_count = route_experts.shape[1]
    capacity = min(tok_count, max(tp_count, 2 * tok_count * top_count // ep_count))
    normed = rms_normed(hidden, norm_gain)
    flat_routes = route_experts.reshape(-1)
    onehot = (flat_routes[:, None] == jnp.arange(ep_count, dtype=jnp.int32)[None, :]).astype(
        jnp.int32
    )
    before = jnp.cumsum(onehot, axis=0) - onehot
    slot_of = jnp.sum(before * onehot, axis=1)
    target = (flat_routes * capacity + slot_of).reshape(tok_count, top_count)
    columns = jnp.arange(ep_count * capacity, dtype=jnp.int32)
    matches = target[:, :, None] == columns[None, None, :]
    placing = jnp.any(matches, axis=1).astype(jnp.bfloat16)
    weighting = jnp.sum(jnp.where(matches, route_weight[:, :, None], 0.0), axis=1)
    outgoing = lax.dot_general(
        placing, normed, (((0,), (0,)), ((), ())), preferred_element_type=jnp.float32
    ).astype(jnp.bfloat16)
    outgoing = outgoing.reshape(ep_count, capacity, model_width)
    gate_up_weight = unpack_rows(gate_up_codes[0], gate_up_scales[0])
    down_weight = unpack_weights(down_codes[0], down_scales[0])
    arrived = lax.all_to_all(outgoing, "ep", split_axis=0, concat_axis=0, tiled=True)
    source_count, item_count, _ = arrived.shape
    flat_rows = arrived.reshape(source_count * item_count, model_width)
    projected = jnp.dot(
        flat_rows, gate_up_weight, preferred_element_type=jnp.float32
    ) + gate_up_bias[0].astype(jnp.float32)
    gate_part = jnp.minimum(projected[:, 0::2], 7.0)
    upward = jnp.clip(projected[:, 1::2], -7.0, 7.0)
    activated = (gate_part * jax.nn.sigmoid(1.702 * gate_part) * (upward + 1.0)).astype(
        jnp.bfloat16
    )
    partial_value = jnp.dot(activated, down_weight, preferred_element_type=jnp.float32)
    partial_value = partial_value.astype(jnp.bfloat16).astype(jnp.float32)
    partial_value = partial_value.reshape(source_count, item_count, model_width)
    summed = lax.psum_scatter(
        partial_value.astype(jnp.bfloat16), "tp", scatter_dimension=2, tiled=True
    ).astype(jnp.float32)
    answered = (summed + down_bias[0].astype(jnp.float32)).astype(jnp.bfloat16)
    came_back = lax.all_to_all(answered, "ep", split_axis=0, concat_axis=0, tiled=True)
    quarter = model_width // tp_count
    own_cols = lax.dynamic_slice_in_dim(hidden, tp_rank * quarter, quarter, 1).astype(jnp.float32)
    gathered = came_back.reshape(ep_count * capacity, quarter).astype(jnp.float32)
    layer_out = own_cols + jnp.dot(weighting, gathered, precision=lax.Precision.HIGHEST)
    return layer_out.astype(jnp.bfloat16)

BF16 = jnp.bfloat16
F32 = jnp.float32
CHUNKS = 2


def word_order(size, lone):
    pos = lax.broadcasted_iota(jnp.int32, (size, size), 1)
    col = lax.broadcasted_iota(jnp.int32, (size, size), 0)
    inner = pos & 63
    source = pos - inner + 8 * (inner & 7) + (inner >> 3)
    if lone:
        last = pos - (size - 32)
        half = size - 32 + 8 * (last & 3) + 2 * (last >> 3) + ((last & 7) >> 2)
        source = jnp.where(last >= 0, half, source)
    return (col == source).astype(F32).astype(BF16)


def matmul(a, b, contract=(1, 0)):
    return lax.dot_general(
        a, b, (((contract[0],), (contract[1],)), ((), ())), preferred_element_type=F32
    )


def column_blocks(total):
    blocks = [(start, 256) for start in range(0, total - total % 256, 256)]
    return blocks + ([(total // 256 * 256, total % 256)] if total % 256 else [])


def decoded(words, quad, negative, scale):
    doubled = lax.shift_right_logical(jnp.full_like(words, MAGNITUDES), quad) & 15
    return doubled.astype(F32) * jnp.where(negative, -scale, scale)


def decode_words(words, scales):
    pieces = []
    for j in range(8):
        moved = jnp.left_shift(words, 2) if j == 0 else lax.shift_right_logical(words, 4 * j - 2)
        negative = (words if j == 7 else jnp.left_shift(words, 28 - 4 * j)) < 0
        pieces.append(decoded(words, moved & 28, negative, scales[j]))
    return jnp.concatenate(pieces, axis=0).astype(BF16)


def layer_kernel(
    sizes,
    hidden,
    routes,
    route_weights,
    gain,
    gate_codes_in,
    gate_scales_in,
    gate_bias,
    down_codes_in,
    down_scales_in,
    down_bias,
    out,
    gate_codes,
    down_codes,
    shifted_codes,
    gate_scales,
    down_scales,
    own_part,
    bias_part,
    rows_in,
    gate_weight,
    down_weight,
    activated,
    pair_out,
    pair_in,
    side_out,
    side_in,
    kept,
    step_out,
    step_in,
    load_sem,
    own_send,
    own_recv,
    line_send,
    line_recv,
    cross_send,
    cross_recv,
    pass_send,
    pass_recv,
    pair_send,
    pair_recv,
    side_send,
    side_recv,
    step_send,
    step_recv,
):
    tok, width, n_z, cuts = sizes
    half_rows = tok // 2
    part_rows = half_rows // CHUNKS
    half_cols = width // 2
    ep = lax.axis_index("ep")
    x = lax.axis_index("tp")
    z = ep // 2
    core = ep % 2
    partner = {"ep": 2 * z + 1 - core}
    across = {"tp": 1 - x}
    beside = z + 1 - 2 * (z % 2)
    beyond = (z + 2) % 4
    neighbour = {"ep": 2 * beside + core}
    opposite = {"ep": 2 * beyond + core}
    along = [{"ep": 2 * ((z + 1) % n_z) + core}, {"ep": 2 * ((z + n_z - 1) % n_z) + core}]

    def copy(src, dst, send, recv, device):
        return pltpu.make_async_remote_copy(
            src_ref=src,
            dst_ref=dst,
            send_sem=send,
            recv_sem=recv,
            device_id=device,
            device_id_type=pl.DeviceIdType.MESH,
        )

    loads = [
        pltpu.make_async_copy(gate_codes_in, gate_codes, load_sem.at[0]),
        pltpu.make_async_copy(down_codes_in, down_codes, load_sem.at[1]),
    ]
    for load in loads:
        load.start()
    barrier = pltpu.get_barrier_semaphore()
    others = [{"ep": 2 * ((z + d) % n_z) + core} for d in range(1, n_z)]
    for device in [partner, across] + others:
        pl.semaphore_signal(
            barrier, inc=1, device_id=device, device_id_type=pl.DeviceIdType.MESH
        )

    order = word_order(256, False)
    blocks = column_blocks(width)
    wide = jnp.concatenate(
        [matmul(hidden[:, c : c + n], order[:n, :n]) for c, n in blocks], axis=1
    )
    gain_row = jnp.concatenate(
        [matmul(gain[:, c : c + n], order[:n, :n]) for c, n in blocks], axis=1
    )
    plain = hidden[...].astype(F32)
    mean_square = jnp.mean(plain * plain, axis=-1, keepdims=True)
    normed = (wide * lax.rsqrt(mean_square + 1e-05) * gain_row).astype(BF16)
    number = lax.broadcasted_iota(jnp.int32, (SPARE, tok), 0)
    weight_at = jnp.zeros((SPARE, tok), F32)
    for k in range(routes.shape[0]):
        chosen = routes[k : k + 1, :] == number % (2 * n_z)
        weight_at = weight_at + jnp.where(chosen, route_weights[k : k + 1, :], 0.0)
    high = weight_at.astype(BF16).astype(F32)
    middle = (weight_at - high).astype(BF16).astype(F32)
    low = weight_at - high - middle
    piece = number // (2 * n_z)
    spare = jnp.where(
        piece == 0, high, jnp.where(piece == 1, middle, jnp.where(piece == 2, low, 0.0))
    )
    same = lax.broadcasted_iota(jnp.int32, (tok, tok), 0) == lax.broadcasted_iota(
        jnp.int32, (tok, tok), 1
    )
    spare_lanes = matmul(same.astype(F32).astype(BF16), spare.astype(BF16), (1, 1))
    aligned = width // 128 * 128
    mine = pl.ds(pl.multiple_of(ep * tok, tok), tok)
    rows_in[mine, :aligned] = normed[:, :aligned]
    rows_in[mine, aligned:] = jnp.concatenate(
        [normed[:, aligned:], spare_lanes.astype(BF16)], axis=1
    )

    pl.semaphore_wait(barrier, n_z + 1)

    def part(chip, half, k):
        start = (2 * chip + core) * tok + half * half_rows + k * part_rows
        return rows_in.at[pl.ds(pl.multiple_of(start, part_rows), part_rows)]

    def line_copy(side, s, k, chip):
        return copy(
            part(chip, x, k),
            part(chip, x, k),
            line_send.at[side, s, k],
            line_recv.at[side, s, k],
            along[side],
        )

    def origin(side, s):
        return (z + n_z - s) % n_z if side == 0 else (z + s) % n_z

    def has(side, s):
        return z >= s if side == 0 else z + s < n_z

    def goes(side):
        return z < n_z - 1 if side == 0 else z > 0

    def both(side, s):
        return (z >= s) & (z < n_z - 1) if side == 0 else (z + s < n_z) & (z > 0)

    for k in range(CHUNKS):
        for side in range(2):

            @pl.when(goes(side))
            def _():
                line_copy(side, 1, k, z).start()

    own_block = rows_in.at[mine]
    own = copy(own_block, own_block, own_send, own_recv, partner)
    own.start()

    def cross_copy(side, s, k):
        ref = part(origin(side, s), x, k)
        return copy(ref, ref, cross_send.at[side, s, k], cross_recv.at[side, s, k], across)

    def pass_copy(side, s, k, i):
        ref = part(origin(side, s), x if i == 0 else 1 - x, k)
        return copy(ref, ref, pass_send.at[side, s, k, i], pass_recv.at[side, s, k, i], partner)

    def arrive(s, k):
        for side in range(2):

            @pl.when(has(side, s))
            def _():
                line_copy(side, s, k, origin(side, s)).wait_recv()
                if s < n_z - 1:

                    @pl.when(goes(side))
                    def _():
                        line_copy(side, s + 1, k, origin(side, s)).start()

                cross_copy(side, s, k).start()
                pass_copy(side, s, k, 0).start()

    def arrive_crossed(s, k):
        for side in range(2):

            @pl.when(has(side, s))
            def _():
                cross_copy(side, s, k).wait_recv()
                pass_copy(side, s, k, 1).start()

    def complete(s):
        for side in range(2):

            @pl.when(has(side, s))
            def _():
                for k in range(CHUNKS):
                    for i in range(2):
                        pass_copy(side, s, k, i).wait_recv()

    def drain(s):
        for side in range(2):

            @pl.when(has(side, s))
            def _():
                for k in range(CHUNKS):
                    cross_copy(side, s, k).wait_send()
                    for i in range(2):
                        pass_copy(side, s, k, i).wait_send()
                    if s < n_z - 1:

                        @pl.when(goes(side))
                        def _():
                            line_copy(side, s + 1, k, origin(side, s)).wait_send()

    gate_scales[...] = gate_scales_in[...].astype(F32) * 0.5
    gate_cols = gate_codes.shape[1]
    col_step = 512 if gate_cols % 512 == 0 else 256
    upper = lax.broadcasted_iota(jnp.int32, (8, col_step), 0) < 4

    def gate_rows(s, carry):
        base = pl.multiple_of(s * 8, 8)
        for col in range(0, gate_cols, col_step):
            words = gate_codes[pl.ds(base, 8), col : col + col_step]
            first, second = (
                jnp.broadcast_to(
                    gate_scales[pl.ds(2 * s + i, 1), col : col + col_step], (8, col_step)
                )
                for i in range(2)
            )
            scale = jnp.where(upper, first, second)
            gate_weight[pl.ds(pl.multiple_of(s * 64, 64), 64), col : col + col_step] = (
                decode_words(words, [scale] * 8)
            )
        return carry

    gate_steps = gate_codes.shape[0] // 8
    gate_weight[pl.ds(width, SPARE), :] = jnp.zeros((SPARE, gate_cols), BF16)
    loads[0].wait()
    marks = [0, 12, 23, 34, gate_steps]
    services = [
        lambda: arrive(1, 0),
        lambda: arrive(1, 1),
        lambda: (arrive(2, 0), arrive_crossed(1, 0)),
        lambda: (arrive(2, 1), arrive_crossed(1, 1)),
    ]
    for low_mark, high_mark, service in zip(marks[:-1], marks[1:], services):
        lax.fori_loop(low_mark, high_mark, gate_rows, 0)
        service()

    scale_rows = down_scales_in.shape[0]
    half_blocks = column_blocks(half_cols)
    tail_size = half_blocks[-1][1]
    tail_order = word_order(tail_size, True)
    for h in range(2):
        for c, n in half_blocks:
            picked = tail_order if n == tail_size else order
            block = down_scales_in[:, h * half_cols + c : h * half_cols + c + n]
            down_scales[h, c : c + n, :scale_rows] = matmul(picked, block, (0, 1)).astype(BF16)
    shown = jnp.where(x == 0, hidden[:, :half_cols], hidden[:, half_cols:])
    for c, n in half_blocks:
        picked = tail_order if n == tail_size else order
        own_part[:, c : c + n] = matmul(shown[:, c : c + n], picked)
        bias_part[:, c : c + n] = matmul(down_bias[:, c : c + n], picked)

    units = down_codes.shape[1]
    words_half = half_cols // 8
    down_steps = words_half // 8
    spread = (
        lax.broadcasted_iota(jnp.int32, (scale_rows, units), 1) // 32
        == lax.broadcasted_iota(jnp.int32, (scale_rows, units), 0)
    ).astype(F32) * 0.5
    spread = spread.astype(BF16)
    loads[1].wait()
    shifted_codes[...] = down_codes[words_half : words_half + down_steps * 8, :]

    def down_rows(h, g, carry):
        base = pl.multiple_of(g * 64, 64)
        source = down_codes if h == 0 else shifted_codes
        start = pl.multiple_of(g * 8, 8)
        scale_block = down_scales[h, pl.ds(base, 64), :scale_rows]
        for col in range(0, units, 256):
            scale = matmul(scale_block, spread[:, col : col + 256])
            words = source[pl.ds(start, 8), col : col + 256]
            down_weight[h, pl.ds(base, 64), col : col + 256] = decode_words(
                words, [scale[8 * j : 8 * j + 8] for j in range(8)]
            )
        return carry

    place = (lax.broadcasted_iota(jnp.int32, (8, units), 0) >> 2) * 4

    def down_last(h):
        base = down_steps * 64
        four = down_codes[h * words_half + down_steps * 8 : (h + 1) * words_half, :]
        words = jnp.concatenate([four, four], axis=0)
        scale = matmul(down_scales[h, base : base + 32, :scale_rows], spread)
        pieces = []
        for i in range(4):
            shift = place + 8 * i
            quad = jnp.left_shift(lax.shift_right_logical(words, shift), 2) & 28
            negative = jnp.left_shift(words, 28 - shift) < 0
            pieces.append(decoded(words, quad, negative, scale[8 * i : 8 * i + 8]))
        down_weight[h, base : base + 32, :] = jnp.concatenate(pieces, axis=0).astype(BF16)

    middle_step = down_steps // 2
    lax.fori_loop(0, middle_step, functools.partial(down_rows, 0), 0)
    arrive(3, 0)
    lax.fori_loop(middle_step, down_steps, functools.partial(down_rows, 0), 0)
    arrive_crossed(2, 0)
    arrive(3, 1)
    lax.fori_loop(0, middle_step, functools.partial(down_rows, 1), 0)
    arrive_crossed(2, 1)
    lax.fori_loop(middle_step, down_steps, functools.partial(down_rows, 1), 0)
    down_last(0)
    down_last(1)
    arrive_crossed(3, 0)
    arrive_crossed(3, 1)

    picks = (
        lax.broadcasted_iota(jnp.int32, (256, 128), 0)
        == 2 * lax.broadcasted_iota(jnp.int32, (256, 128), 1)
    ).astype(F32).astype(BF16)
    batch_rows = 4 * tok
    near = z // 2
    place_in = z % 2
    starts = [pl.multiple_of((1 - near) * batch_rows, batch_rows),
              pl.multiple_of(near * batch_rows, batch_rows)]

    def gate_tile(b, t, carry):
        cols = pl.ds(pl.multiple_of(t * 256, 256), 256)
        projected = jnp.dot(
            rows_in[pl.ds(starts[b], batch_rows), :],
            gate_weight[:, cols],
            preferred_element_type=F32,
        ) + gate_bias[:, cols].astype(F32)
        gate_part = jnp.minimum(projected, 7.0)
        upward = pltpu.roll(jnp.clip(projected, -7.0, 7.0), 255, 1)
        value = gate_part * jax.nn.sigmoid(1.702 * gate_part) * (upward + 1.0)
        activated[b, :, pl.ds(pl.multiple_of(t * 128, 128), 128)] = jnp.dot(
            value.astype(BF16), picks, preferred_element_type=F32
        ).astype(BF16)
        return carry

    def sections(ref, b, h, q):
        c, n = cuts[q]
        return ref.at[b, h, :, :, pl.ds(c, n)]

    def pair_copy(b, h, q):
        return copy(
            sections(pair_out, b, h, q),
            sections(pair_in, b, h, q),
            pair_send.at[b, h, q],
            pair_recv.at[b, h, q],
            partner,
        )

    def side_copy(b, q):
        c, n = cuts[q]
        return copy(
            side_out.at[b, :, :, pl.ds(c, n)],
            side_in.at[b, :, :, pl.ds(c, n)],
            side_send.at[b, q],
            side_recv.at[b, q],
            across,
        )

    def step_copy(i, q):
        c, n = cuts[q]
        return copy(
            step_out.at[i, :, pl.ds(c, n)],
            step_in.at[i, :, pl.ds(c, n)],
            step_send.at[i, q],
            step_recv.at[i, q],
            opposite if i == 1 else neighbour,
        )

    tail = lax.broadcasted_iota(jnp.int32, (batch_rows, SPARE), 1)

    def weights_of(b):
        extra = rows_in[pl.ds(starts[b], batch_rows), width:].astype(F32)
        hit = (tail == ep) | (tail == ep + 2 * n_z) | (tail == ep + 4 * n_z)
        return jnp.sum(jnp.where(hit, extra, 0.0), axis=1, keepdims=True)

    def multiply(b, h, q, weight):
        c, n = cuts[q]
        which = 1 - x if h == 0 else x
        value = matmul(activated[b], down_weight[which, c : c + n, :], (1, 1))
        if h == 1:
            value = value + bias_part[:, c : c + n]
        value = value * weight
        for i in range(2):
            first = value[2 * i * tok : (2 * i + 1) * tok]
            second = value[(2 * i + 1) * tok : (2 * i + 2) * tok]
            pair_out[b, h, i, :, c : c + n] = jnp.where(core == 0, second, first).astype(BF16)
            kept[b, h, i, :, c : c + n] = jnp.where(core == 0, first, second).astype(BF16)
        pair_copy(b, h, q).start()

    def fold_pair(b, h, q):
        c, n = cuts[q]
        pair_copy(b, h, q).wait_recv()
        total = kept[b, h, :, :, c : c + n].astype(F32) + pair_in[
            b, h, :, :, c : c + n
        ].astype(F32)
        if h == 0:
            side_out[b, :, :, c : c + n] = total.astype(BF16)
            side_copy(b, q).start()
        else:
            kept[b, h, :, :, c : c + n] = total.astype(BF16)

    def folded(b, i, q):
        c, n = cuts[q]
        return kept[b, 1, i, :, c : c + n].astype(F32) + side_in[b, i, :, c : c + n].astype(F32)

    def fold_side(b, q):
        c, n = cuts[q]
        side_copy(b, q).wait_recv()
        step_out[0 if b == 0 else 2, :, c : c + n] = folded(b, 1 - place_in, q).astype(BF16)
        step_copy(0 if b == 0 else 2, q).start()

    def fold_step(q):
        c, n = cuts[q]
        step_copy(0, q).wait_recv()
        total = folded(0, place_in, q) + step_in[0, :, c : c + n].astype(F32)
        step_out[1, :, c : c + n] = total.astype(BF16)
        step_copy(1, q).start()

    own.wait_recv()
    for s in range(1, n_z):
        complete(s)
    gate_tiles = gate_cols // 256
    lax.fori_loop(0, gate_tiles, functools.partial(gate_tile, 0), 0)
    far_weight = weights_of(0)
    multiply(0, 0, 0, far_weight)
    multiply(0, 0, 1, far_weight)
    fold_pair(0, 0, 0)
    multiply(0, 1, 0, far_weight)
    fold_pair(0, 0, 1)
    multiply(0, 1, 1, far_weight)
    fold_pair(0, 1, 0)
    lax.fori_loop(0, gate_tiles // 2, functools.partial(gate_tile, 1), 0)
    fold_pair(0, 1, 1)
    fold_side(0, 0)
    lax.fori_loop(gate_tiles // 2, gate_tiles, functools.partial(gate_tile, 1), 0)
    near_weight = weights_of(1)
    multiply(1, 0, 0, near_weight)
    fold_side(0, 1)
    multiply(1, 0, 1, near_weight)
    fold_pair(1, 0, 0)
    fold_step(0)
    multiply(1, 1, 0, near_weight)
    fold_pair(1, 0, 1)
    fold_step(1)
    multiply(1, 1, 1, near_weight)
    fold_pair(1, 1, 0)
    fold_pair(1, 1, 1)
    for q in range(2):
        fold_side(1, q)
    for q, (c, n) in enumerate(cuts):
        total = own_part[:, c : c + n] + folded(1, place_in, q)
        step_copy(1, q).wait_recv()
        total = total + step_in[1, :, c : c + n].astype(F32)
        step_copy(2, q).wait_recv()
        total = total + step_in[2, :, c : c + n].astype(F32)
        own_part[:, c : c + n] = total
    for c, n in half_blocks:
        picked = tail_order if n == tail_size else order
        out[:, c : c + n] = matmul(own_part[:, c : c + n].astype(BF16), picked, (1, 1)).astype(BF16)

    own.wait_send()
    for side in range(2):

        @pl.when(goes(side))
        def _():
            for k in range(CHUNKS):
                line_copy(side, 1, k, z).wait_send()

    for s in range(1, n_z):
        drain(s)
    for q in range(2):
        for b in range(2):
            for h in range(2):
                pair_copy(b, h, q).wait_send()
            side_copy(b, q).wait_send()
        for i in range(3):
            step_copy(i, q).wait_send()


def dense_shards(
    hidden,
    route_experts,
    route_weight,
    norm_gain,
    gate_up_codes,
    gate_up_scales,
    gate_up_bias,
    down_codes,
    down_scales,
    down_bias,
):
    ep_count = lax.axis_size("ep")
    tok, width = hidden.shape
    n_z = ep_count // 2
    half = width // 2
    units = down_codes.shape[1]
    first_cut = -(-half // 256) * 128
    cuts = ((0, first_cut), (first_cut, half - first_cut))
    dma = pltpu.SemaphoreType.DMA
    vmem = pltpu.VMEM
    in_vmem, anywhere = pl.BlockSpec(memory_space=vmem), pl.BlockSpec(memory_space=pl.ANY)
    return pl.pallas_call(
        functools.partial(layer_kernel, (tok, width, n_z, cuts)),
        out_shape=jax.ShapeDtypeStruct((tok, half), BF16),
        in_specs=[in_vmem] * 4 + [anywhere] + [in_vmem] * 2 + [anywhere] + [in_vmem] * 2,
        out_specs=in_vmem,
        scratch_shapes=[
            vmem(gate_up_codes.shape[1:], jnp.int32),
            vmem((down_codes.shape[2], units), jnp.int32),
            vmem((half // 64 * 8, units), jnp.int32),
            vmem(gate_up_scales.shape[1:], F32),
            vmem((2, half, 128), BF16),
            vmem((tok, half), F32),
            vmem((1, half), F32),
            vmem((ep_count * tok, width + SPARE), BF16),
            vmem((width + SPARE, gate_up_codes.shape[2]), BF16),
            vmem((2, half, units), BF16),
            vmem((2, ep_count * tok // 2, units), BF16),
            vmem((2, 2, 2, tok, half), BF16),
            vmem((2, 2, 2, tok, half), BF16),
            vmem((2, 2, tok, half), BF16),
            vmem((2, 2, tok, half), BF16),
            vmem((2, 2, 2, tok, half), BF16),
            vmem((3, tok, half), BF16),
            vmem((3, tok, half), BF16),
            dma((2,)),
            dma,
            dma,
            dma((2, n_z, CHUNKS)),
            dma((2, n_z, CHUNKS)),
            dma((2, n_z, CHUNKS)),
            dma((2, n_z, CHUNKS)),
            dma((2, n_z, CHUNKS, 2)),
            dma((2, n_z, CHUNKS, 2)),
            dma((2, 2, 2)),
            dma((2, 2, 2)),
            dma((2, 2)),
            dma((2, 2)),
            dma((3, 2)),
            dma((3, 2)),
        ],
        compiler_params=pltpu.CompilerParams(
            collective_id=0, has_side_effects=True, vmem_limit_bytes=63 * 1024 * 1024
        ),
    )(
        hidden,
        route_experts.T,
        route_weight.T,
        norm_gain.reshape(1, width),
        gate_up_codes[0],
        gate_up_scales[0],
        gate_up_bias,
        down_codes[0].T,
        down_scales[0],
        down_bias,
    )


def solution(mesh):
    def layer(*arrays):
        tok, top = arrays[1].shape
        ep_count, tp_count = lax.axis_size("ep"), lax.axis_size("tp")
        dense = 2 * top >= ep_count and tp_count == 2 and ep_count == 8 and tok == 64
        return (dense_shards if dense else shards)(*arrays)

    placed = (
        P(("groups", "ep"), None),
        P(("groups", "ep"), None),
        P(("groups", "ep"), None),
        P(),
        P("ep", None, "tp"),
        P("ep", None, "tp"),
        P("ep", "tp"),
        P("ep", "tp", None),
        P("ep", "tp", None),
        P("ep", "tp"),
    )
    return jax.shard_map(
        layer, mesh=mesh, in_specs=placed, out_specs=P(("groups", "ep"), "tp"), check_vma=False
    )
```

```python
import functools

import jax
import jax.numpy as jnp
from jax import lax
from jax.experimental import pallas as pl
from jax.experimental.pallas import tpu as pltpu
from jax.sharding import PartitionSpec as P

MAGNITUDES = 0xC8643210 - (1 << 32)
SPARE = 64


def decode_nibble(nibble):
    magnit = nibble & 7
    exponent = jnp.maximum(jnp.right_shift(magnit, 1) - 1, 0)
    doubled = jnp.where(magnit < 2, magnit, jnp.left_shift(2 + (magnit & 1), exponent))
    signed_val = doubled.astype(jnp.float32) * 0.5
    return jnp.where(nibble >= 8, -signed_val, signed_val)


def unpack_weights(packed, scaling):
    row_count = packed.shape[0]
    shifts = jnp.arange(8, dtype=jnp.int32) * 4
    nibble = jnp.right_shift(packed[:, :, None], shifts[None, None, :]) & 15
    nibble = nibble.reshape(row_count, packed.shape[1] * 8)
    signed_val = decode_nibble(nibble)
    signed_val = (
        signed_val.reshape(row_count // 32, 32, -1) * scaling.astype(jnp.float32)[:, None, :]
    )
    return signed_val.reshape(row_count, -1).astype(jnp.bfloat16)


def unpack_rows(packed, scaling):
    row_count = packed.shape[0] * 8
    shifts = jnp.arange(8, dtype=jnp.int32) * 4
    nibble = jnp.right_shift(packed[:, None, :], shifts[None, :, None]) & 15
    nibble = nibble.reshape(row_count, packed.shape[1])
    signed_val = decode_nibble(nibble)
    signed_val = (
        signed_val.reshape(row_count // 32, 32, -1) * scaling.astype(jnp.float32)[:, None, :]
    )
    return signed_val.reshape(row_count, -1).astype(jnp.bfloat16)


def rms_normed(hidden, norm_gain):
    widened = hidden.astype(jnp.float32)
    mean_square = jnp.mean(widened * widened, axis=-1, keepdims=True)
    scaled = widened * lax.rsqrt(mean_square + 1e-05) * norm_gain.astype(jnp.float32)
    return scaled.astype(jnp.bfloat16)


def shards(
    hidden,
    route_experts,
    route_weight,
    norm_gain,
    gate_up_codes,
    gate_up_scales,
    gate_up_bias,
    down_codes,
    down_scales,
    down_bias,
):
    ep_count = lax.axis_size("ep")
    tp_count = lax.axis_size("tp")
    tp_rank = lax.axis_index("tp")
    tok_count, model_width = hidden.shape
    top_count = route_experts.shape[1]
    capacity = min(tok_count, max(tp_count, 2 * tok_count * top_count // ep_count))
    normed = rms_normed(hidden, norm_gain)
    flat_routes = route_experts.reshape(-1)
    onehot = (flat_routes[:, None] == jnp.arange(ep_count, dtype=jnp.int32)[None, :]).astype(
        jnp.int32
    )
    before = jnp.cumsum(onehot, axis=0) - onehot
    slot_of = jnp.sum(before * onehot, axis=1)
    target = (flat_routes * capacity + slot_of).reshape(tok_count, top_count)
    columns = jnp.arange(ep_count * capacity, dtype=jnp.int32)
    matches = target[:, :, None] == columns[None, None, :]
    placing = jnp.any(matches, axis=1).astype(jnp.bfloat16)
    weighting = jnp.sum(jnp.where(matches, route_weight[:, :, None], 0.0), axis=1)
    outgoing = lax.dot_general(
        placing, normed, (((0,), (0,)), ((), ())), preferred_element_type=jnp.float32
    ).astype(jnp.bfloat16)
    outgoing = outgoing.reshape(ep_count, capacity, model_width)
    gate_up_weight = unpack_rows(gate_up_codes[0], gate_up_scales[0])
    down_weight = unpack_weights(down_codes[0], down_scales[0])
    arrived = lax.all_to_all(outgoing, "ep", split_axis=0, concat_axis=0, tiled=True)
    source_count, item_count, _ = arrived.shape
    flat_rows = arrived.reshape(source_count * item_count, model_width)
    projected = jnp.dot(
        flat_rows, gate_up_weight, preferred_element_type=jnp.float32
    ) + gate_up_bias[0].astype(jnp.float32)
    gate_part = jnp.minimum(projected[:, 0::2], 7.0)
    upward = jnp.clip(projected[:, 1::2], -7.0, 7.0)
    activated = (gate_part * jax.nn.sigmoid(1.702 * gate_part) * (upward + 1.0)).astype(
        jnp.bfloat16
    )
    partial_value = jnp.dot(activated, down_weight, preferred_element_type=jnp.float32)
    partial_value = partial_value.astype(jnp.bfloat16).astype(jnp.float32)
    partial_value = partial_value.reshape(source_count, item_count, model_width)
    summed = lax.psum_scatter(
        partial_value.astype(jnp.bfloat16), "tp", scatter_dimension=2, tiled=True
    ).astype(jnp.float32)
    answered = (summed + down_bias[0].astype(jnp.float32)).astype(jnp.bfloat16)
    came_back = lax.all_to_all(answered, "ep", split_axis=0, concat_axis=0, tiled=True)
    quarter = model_width // tp_count
    own_cols = lax.dynamic_slice_in_dim(hidden, tp_rank * quarter, quarter, 1).astype(jnp.float32)
    gathered = came_back.reshape(ep_count * capacity, quarter).astype(jnp.float32)
    layer_out = own_cols + jnp.dot(weighting, gathered, precision=lax.Precision.HIGHEST)
    return layer_out.astype(jnp.bfloat16)

BF16 = jnp.bfloat16
F32 = jnp.float32
CHUNKS = 2


def word_order(size, lone):
    pos = lax.broadcasted_iota(jnp.int32, (size, size), 1)
    col = lax.broadcasted_iota(jnp.int32, (size, size), 0)
    inner = pos & 63
    source = pos - inner + 8 * (inner & 7) + (inner >> 3)
    if lone:
        last = pos - (size - 32)
        half = size - 32 + 8 * (last & 3) + 2 * (last >> 3) + ((last & 7) >> 2)
        source = jnp.where(last >= 0, half, source)
    return (col == source).astype(F32).astype(BF16)


def matmul(a, b, contract=(1, 0)):
    return lax.dot_general(
        a, b, (((contract[0],), (contract[1],)), ((), ())), preferred_element_type=F32
    )


def column_blocks(total):
    blocks = [(start, 256) for start in range(0, total - total % 256, 256)]
    return blocks + ([(total // 256 * 256, total % 256)] if total % 256 else [])


def magnitude(words, quad):
    return (lax.shift_right_logical(jnp.full_like(words, MAGNITUDES), quad) & 15).astype(F32)


def decode_words(words, scales):
    pieces = []
    for quarter in range(4):
        j = 2 * quarter
        upper = words if j < 4 else lax.shift_right_logical(words, 16)
        pair = jnp.concatenate([upper, lax.shift_right_logical(words, 4 + j // 4 * 16)], axis=0)
        negative = (pair.astype(jnp.int16) & jnp.int16(8 << (4 * (j % 4)))) != 0
        sizes = []
        for i in (j, j + 1):
            moved = jnp.left_shift(words, 2) if i == 0 else lax.shift_right_logical(words, 4 * i - 2)
            sizes.append(magnitude(words, moved & 28))
        scale = scales[quarter]
        pieces.append(
            jnp.concatenate(sizes, axis=0).astype(BF16) * jnp.where(negative, -scale, scale)
        )
    return jnp.concatenate(pieces, axis=0)


def layer_kernel(
    sizes,
    hidden,
    routes,
    route_weights,
    gain,
    gate_codes_in,
    gate_scales_in,
    gate_bias,
    down_codes_in,
    down_scales_in,
    down_bias,
    out,
    gate_codes,
    down_codes,
    shifted_codes,
    gate_scales,
    down_scales,
    own_part,
    bias_part,
    rows_in,
    gate_weight,
    down_weight,
    activated,
    pair_out,
    pair_in,
    side_out,
    side_in,
    kept,
    step_out,
    step_in,
    load_sem,
    own_send,
    own_recv,
    line_send,
    line_recv,
    cross_send,
    cross_recv,
    pass_send,
    pass_recv,
    pair_send,
    pair_recv,
    side_send,
    side_recv,
    step_send,
    step_recv,
):
    tok, width, n_z, cuts = sizes
    half_rows = tok // 2
    part_rows = half_rows // CHUNKS
    half_cols = width // 2
    ep = lax.axis_index("ep")
    x = lax.axis_index("tp")
    z = ep // 2
    core = ep % 2
    partner = {"ep": 2 * z + 1 - core}
    across = {"tp": 1 - x}
    beside = z + 1 - 2 * (z % 2)
    beyond = (z + 2) % 4
    neighbour = {"ep": 2 * beside + core}
    opposite = {"ep": 2 * beyond + core}

    def copy(src, dst, send, recv, device):
        return pltpu.make_async_remote_copy(
            src_ref=src,
            dst_ref=dst,
            send_sem=send,
            recv_sem=recv,
            device_id=device,
            device_id_type=pl.DeviceIdType.MESH,
        )

    loads = [
        pltpu.make_async_copy(gate_codes_in, gate_codes, load_sem.at[0]),
        pltpu.make_async_copy(down_codes_in, down_codes, load_sem.at[1]),
    ]
    for load in loads:
        load.start()
    barrier = pltpu.get_barrier_semaphore()
    others = [{"ep": 2 * ((z + d) % n_z) + core} for d in range(1, n_z)]
    for device in [partner, across] + others:
        pl.semaphore_signal(
            barrier, inc=1, device_id=device, device_id_type=pl.DeviceIdType.MESH
        )

    order = word_order(256, False)
    blocks = column_blocks(width)
    wide = jnp.concatenate(
        [matmul(hidden[:, c : c + n], order[:n, :n]) for c, n in blocks], axis=1
    )
    gain_row = jnp.concatenate(
        [matmul(gain[:, c : c + n], order[:n, :n]) for c, n in blocks], axis=1
    )
    plain = hidden[...].astype(F32)
    mean_square = jnp.mean(plain * plain, axis=-1, keepdims=True)
    normed = (wide * lax.rsqrt(mean_square + 1e-05) * gain_row).astype(BF16)
    number = lax.broadcasted_iota(jnp.int32, (SPARE, tok), 0)
    weight_at = jnp.zeros((SPARE, tok), F32)
    for k in range(routes.shape[0]):
        chosen = routes[k : k + 1, :] == number % (2 * n_z)
        weight_at = weight_at + jnp.where(chosen, route_weights[k : k + 1, :], 0.0)
    high = weight_at.astype(BF16).astype(F32)
    middle = (weight_at - high).astype(BF16).astype(F32)
    low = weight_at - high - middle
    piece = number // (2 * n_z)
    spare = jnp.where(
        piece == 0, high, jnp.where(piece == 1, middle, jnp.where(piece == 2, low, 0.0))
    )
    same = lax.broadcasted_iota(jnp.int32, (tok, tok), 0) == lax.broadcasted_iota(
        jnp.int32, (tok, tok), 1
    )
    spare_lanes = matmul(same.astype(F32).astype(BF16), spare.astype(BF16), (1, 1))
    aligned = width // 128 * 128
    mine = pl.ds(pl.multiple_of(ep * tok, tok), tok)
    rows_in[mine, :aligned] = normed[:, :aligned]
    rows_in[mine, aligned:] = jnp.concatenate(
        [normed[:, aligned:], spare_lanes.astype(BF16)], axis=1
    )

    pl.semaphore_wait(barrier, n_z + 1)

    def part(chip, half, k):
        start = (2 * chip + core) * tok + half * half_rows + k * part_rows
        return rows_in.at[pl.ds(pl.multiple_of(start, part_rows), part_rows)]

    near = 1 - z % 2

    def origin(side, s):
        return (z + n_z + (2 * side - 1) * s) % n_z

    def has(side, s):
        return side * (n_z - 1 - z) + (1 - side) * z >= s

    def goes(side):
        return side * z + (1 - side) * (n_z - 1 - z) >= 1

    def line_copy(side, s, k, chip):
        ref = part(chip, x, k)
        onward = {"ep": 2 * ((z + n_z + 1 - 2 * side) % n_z) + core}
        return copy(ref, ref, line_send.at[side, s, k], line_recv.at[side, s, k], onward)

    def cross_copy(side, s, k):
        ref = part(origin(side, s), x, k)
        return copy(ref, ref, cross_send.at[side, s, k], cross_recv.at[side, s, k], across)

    def pass_copy(side, s, k, i):
        ref = part(origin(side, s), x if i == 0 else 1 - x, k)
        return copy(ref, ref, pass_send.at[side, s, k, i], pass_recv.at[side, s, k, i], partner)

    def when(condition, action):
        pl.when(condition)(action)

    for k in range(CHUNKS):
        for side in range(2):
            when(goes(side), lambda: line_copy(side, 1, k, z).start())

    own_block = rows_in.at[mine]
    own = copy(own_block, own_block, own_send, own_recv, partner)
    own.start()

    def arrive(side, s, k):
        def action():
            line_copy(side, s, k, origin(side, s)).wait_recv()
            if s < n_z - 1:
                when(goes(side), lambda: line_copy(side, s + 1, k, origin(side, s)).start())
            pass_copy(side, s, k, 0).start()

        when(has(side, s), action)

    def cross(side, s, k):
        when(has(side, s), lambda: cross_copy(side, s, k).start())

    def arrive_crossed(side, s, k):
        def action():
            cross_copy(side, s, k).wait_recv()
            pass_copy(side, s, k, 1).start()

        when(has(side, s), action)

    def complete(side, s):
        def action():
            for k in range(CHUNKS):
                for i in range(2):
                    pass_copy(side, s, k, i).wait_recv()

        when(has(side, s), action)

    def drain(side, s):
        def action():
            for k in range(CHUNKS):
                cross_copy(side, s, k).wait_send()
                for i in range(2):
                    pass_copy(side, s, k, i).wait_send()
                if s < n_z - 1:
                    when(
                        goes(side),
                        lambda: line_copy(side, s + 1, k, origin(side, s)).wait_send(),
                    )

        when(has(side, s), action)

    far = 1 - near

    def first_arrives(k):
        arrive(near, 1, k)
        arrive(far, 1, k)
        cross(near, 1, k)

    def later_arrives(s, k):
        arrive(near, s, k)
        arrive(far, s, k)
        cross(near, s, k)
        cross(far, s, k)

    def crossed(s, k):
        arrive_crossed(near, s, k)
        arrive_crossed(far, s, k)

    gate_scales[...] = gate_scales_in[...].astype(F32) * 0.5
    gate_cols = gate_codes.shape[1]
    col_step = 512 if gate_cols % 512 == 0 else 256
    upper = lax.broadcasted_iota(jnp.int32, (16, col_step), 0) % 8 < 4

    def gate_rows(s, carry):
        base = pl.multiple_of(s * 8, 8)
        for col in range(0, gate_cols, col_step):
            words = gate_codes[pl.ds(base, 8), col : col + col_step]
            first, second = (
                jnp.broadcast_to(
                    gate_scales[pl.ds(2 * s + i, 1), col : col + col_step], (16, col_step)
                )
                for i in range(2)
            )
            scale = jnp.where(upper, first, second).astype(BF16)
            gate_weight[pl.ds(pl.multiple_of(s * 64, 64), 64), col : col + col_step] = (
                decode_words(words, [scale] * 4)
            )
        return carry

    gate_steps = gate_codes.shape[0] // 8
    gate_weight[pl.ds(width, SPARE), :] = jnp.zeros((SPARE, gate_cols), BF16)
    loads[0].wait()
    marks = [0, gate_steps * 24 // 45, gate_steps * 35 // 45, gate_steps]
    lax.fori_loop(marks[0], marks[1], gate_rows, 0)
    first_arrives(0)
    lax.fori_loop(marks[1], marks[2], gate_rows, 0)
    first_arrives(1)
    for k in range(CHUNKS):
        cross(far, 1, k)
    lax.fori_loop(marks[2], marks[3], gate_rows, 0)
    later_arrives(2, 0)
    arrive_crossed(near, 1, 0)

    scale_rows = down_scales_in.shape[0]
    half_blocks = column_blocks(half_cols)
    tail_size = half_blocks[-1][1]
    tail_order = word_order(tail_size, True)
    for h in range(2):
        for c, n in half_blocks:
            picked = tail_order if n == tail_size else order
            block = down_scales_in[:, h * half_cols + c : h * half_cols + c + n]
            down_scales[h, c : c + n, :scale_rows] = matmul(picked, block, (0, 1)).astype(BF16)
    shown = jnp.where(x == 0, hidden[:, :half_cols], hidden[:, half_cols:])
    for c, n in half_blocks:
        picked = tail_order if n == tail_size else order
        own_part[:, c : c + n] = matmul(shown[:, c : c + n], picked)
        bias_part[:, c : c + n] = matmul(down_bias[:, c : c + n], picked)

    units = down_codes.shape[1]
    words_half = half_cols // 8
    down_steps = words_half // 8
    spread = (
        lax.broadcasted_iota(jnp.int32, (scale_rows, units), 1) // 32
        == lax.broadcasted_iota(jnp.int32, (scale_rows, units), 0)
    ).astype(F32) * 0.5
    spread = spread.astype(BF16)
    loads[1].wait()
    shifted_codes[...] = down_codes[words_half : words_half + down_steps * 8, :]

    def down_rows(h, g, carry):
        base = pl.multiple_of(g * 128, 128)
        source = down_codes if h == 0 else shifted_codes
        scale_block = down_scales[h, pl.ds(base, 128), :scale_rows]
        for col in range(0, units, 256):
            scale = matmul(scale_block, spread[:, col : col + 256]).astype(BF16)
            for i in range(2):
                words = source[pl.ds(pl.multiple_of(g * 16 + 8 * i, 8), 8), col : col + 256]
                start = pl.multiple_of(base + 64 * i, 64)
                down_weight[h, pl.ds(start, 64), col : col + 256] = decode_words(
                    words, [scale[64 * i + 16 * j : 64 * i + 16 * j + 16] for j in range(4)]
                )
        return carry

    place = (lax.broadcasted_iota(jnp.int32, (8, units), 0) >> 2) * 4

    def down_last(h):
        base = down_steps * 64
        four = down_codes[h * words_half + down_steps * 8 : (h + 1) * words_half, :]
        words = jnp.concatenate([four, four], axis=0)
        scale = matmul(down_scales[h, base : base + 32, :scale_rows], spread)
        pieces = []
        for i in range(4):
            shift = place + 8 * i
            quad = jnp.left_shift(lax.shift_right_logical(words, shift), 2) & 28
            negative = jnp.left_shift(words, 28 - shift) < 0
            part_scale = scale[8 * i : 8 * i + 8]
            pieces.append(magnitude(words, quad) * jnp.where(negative, -part_scale, part_scale))
        down_weight[h, base : base + 32, :] = jnp.concatenate(pieces, axis=0).astype(BF16)

    pair_steps = down_steps // 2
    middle_step = pair_steps // 2
    lax.fori_loop(0, middle_step, functools.partial(down_rows, 0), 0)
    later_arrives(2, 1)
    arrive_crossed(near, 1, 1)
    lax.fori_loop(middle_step, pair_steps, functools.partial(down_rows, 0), 0)
    arrive_crossed(far, 1, 0)
    lax.fori_loop(0, middle_step, functools.partial(down_rows, 1), 0)
    later_arrives(3, 0)
    lax.fori_loop(middle_step, pair_steps, functools.partial(down_rows, 1), 0)
    arrive_crossed(far, 1, 1)
    crossed(2, 0)
    down_last(0)
    down_last(1)

    picks = (
        lax.broadcasted_iota(jnp.int32, (256, 128), 0)
        == 2 * lax.broadcasted_iota(jnp.int32, (256, 128), 1)
    ).astype(F32).astype(BF16)
    batch_rows = 4 * tok
    group = z // 2
    place_in = z % 2
    starts = [
        pl.multiple_of(group * batch_rows, batch_rows),
        pl.multiple_of((1 - group) * batch_rows, batch_rows),
    ]
    tile_cols = gate_cols // 2

    def gate_tile(b, t):
        projected = jnp.dot(
            rows_in[pl.ds(starts[b], batch_rows), :],
            gate_weight[:, t * tile_cols : (t + 1) * tile_cols],
            preferred_element_type=F32,
        ) + gate_bias[:, t * tile_cols : (t + 1) * tile_cols].astype(F32)
        gate_part = jnp.minimum(projected, 7.0)
        upward = pltpu.roll(jnp.clip(projected, -7.0, 7.0), tile_cols - 1, 1)
        value = (gate_part * jax.nn.sigmoid(1.702 * gate_part) * (upward + 1.0)).astype(BF16)
        for c in range(0, tile_cols, 256):
            at = (t * tile_cols + c) // 2
            activated[b, :, at : at + 128] = matmul(value[:, c : c + 256], picks).astype(BF16)

    def pair_copy(b, h, q):
        c, n = cuts[q]
        return copy(
            pair_out.at[b, h, :, :, pl.ds(c, n)],
            pair_in.at[b, h, :, :, pl.ds(c, n)],
            pair_send.at[b, h, q],
            pair_recv.at[b, h, q],
            partner,
        )

    def side_copy(b, q):
        c, n = cuts[q]
        return copy(
            side_out.at[b, :, :, pl.ds(c, n)],
            side_in.at[b, :, :, pl.ds(c, n)],
            side_send.at[b, q],
            side_recv.at[b, q],
            across,
        )

    def step_copy(i, q):
        c, n = cuts[q]
        return copy(
            step_out.at[i, :, pl.ds(c, n)],
            step_in.at[i, :, pl.ds(c, n)],
            step_send.at[i, q],
            step_recv.at[i, q],
            opposite if i == 2 else neighbour,
        )

    tail = lax.broadcasted_iota(jnp.int32, (batch_rows, SPARE), 1)

    def weights_of(b):
        extra = rows_in[pl.ds(starts[b], batch_rows), width:].astype(F32)
        hit = (tail == ep) | (tail == ep + 2 * n_z) | (tail == ep + 4 * n_z)
        return jnp.sum(jnp.where(hit, extra, 0.0), axis=1, keepdims=True)

    parts = range(len(cuts))

    def multiply(b, h, weight):
        which = 1 - x if h == 0 else x
        value = matmul(activated[b], down_weight[which], (1, 1))
        if h == 1:
            value = value + bias_part[...]
        value = value * weight
        for i in range(2):
            first = value[2 * i * tok : (2 * i + 1) * tok]
            second = value[(2 * i + 1) * tok : (2 * i + 2) * tok]
            pair_out[b, h, i] = jnp.where(core == 0, second, first).astype(BF16)
            kept[b, h, i] = jnp.where(core == 0, first, second).astype(BF16)
        for q in parts:
            pair_copy(b, h, q).start()

    def fold_pair(b, h, q):
        c, n = cuts[q]
        pair_copy(b, h, q).wait_recv()
        total = kept[b, h, :, :, c : c + n].astype(F32) + pair_in[
            b, h, :, :, c : c + n
        ].astype(F32)
        if h == 0:
            side_out[b, :, :, c : c + n] = total.astype(BF16)
            side_copy(b, q).start()
        else:
            kept[b, h, :, :, c : c + n] = total.astype(BF16)

    def folded(b, i, q):
        c, n = cuts[q]
        return kept[b, 1, i, :, c : c + n].astype(F32) + side_in[b, i, :, c : c + n].astype(F32)

    def fold_side(b, q):
        c, n = cuts[q]
        side_copy(b, q).wait_recv()
        step_out[b, :, c : c + n] = folded(b, 1 - place_in, q).astype(BF16)
        step_copy(b, q).start()
        if b == 0:
            own_part[:, c : c + n] = own_part[:, c : c + n] + folded(0, place_in, q)

    def fold_step(q):
        c, n = cuts[q]
        step_copy(1, q).wait_recv()
        total = folded(1, place_in, q) + step_in[1, :, c : c + n].astype(F32)
        step_out[2, :, c : c + n] = total.astype(BF16)
        step_copy(2, q).start()

    def add_step(i, q):
        c, n = cuts[q]
        step_copy(i, q).wait_recv()
        own_part[:, c : c + n] = own_part[:, c : c + n] + step_in[i, :, c : c + n].astype(F32)

    def write_out(q):
        c, n = cuts[q]
        at = c
        while at < c + n:
            left = half_cols - at
            size = tail_size if left == tail_size else min(256, c + n - at)
            if left > tail_size and left - size < tail_size:
                size = left - tail_size
            picked = tail_order if left == tail_size else order[:size, :size]
            block = own_part[:, at : at + size].astype(BF16)
            out[:, at : at + size] = matmul(block, picked, (1, 1)).astype(BF16)
            at += size

    own.wait_recv()
    complete(near, 1)
    near_weight = weights_of(0)
    gate_tile(0, 0)
    later_arrives(3, 1)
    crossed(2, 1)
    gate_tile(0, 1)
    crossed(3, 0)
    multiply(0, 0, near_weight)
    crossed(3, 1)
    multiply(0, 1, near_weight)
    for q in parts:
        fold_pair(0, 0, q)
    for q in parts:
        fold_pair(0, 1, q)
    complete(far, 1)
    for s in range(2, n_z):
        complete(0, s)
        complete(1, s)
    far_weight = weights_of(1)
    gate_tile(1, 0)
    for q in (0, 1):
        fold_side(0, q)
    gate_tile(1, 1)
    multiply(1, 0, far_weight)
    fold_side(0, 2)
    for q in parts:
        fold_pair(1, 0, q)
    multiply(1, 1, far_weight)
    fold_side(0, 3)
    for q in parts:
        fold_pair(1, 1, q)
    for q in parts:
        add_step(0, q)
    for q in parts:
        fold_side(1, q)
        if q:
            fold_step(q - 1)
    fold_step(len(cuts) - 1)
    for q in parts:
        add_step(2, q)
        write_out(q)

    own.wait_send()
    for side in range(2):

        def sent():
            for k in range(CHUNKS):
                line_copy(side, 1, k, z).wait_send()

        when(goes(side), sent)
        for s in range(1, n_z):
            drain(side, s)
    for q in parts:
        for b in range(2):
            for h in range(2):
                pair_copy(b, h, q).wait_send()
            side_copy(b, q).wait_send()
        for i in range(3):
            step_copy(i, q).wait_send()


def dense_shards(
    hidden,
    route_experts,
    route_weight,
    norm_gain,
    gate_up_codes,
    gate_up_scales,
    gate_up_bias,
    down_codes,
    down_scales,
    down_bias,
):
    ep_count = lax.axis_size("ep")
    tok, width = hidden.shape
    n_z = ep_count // 2
    half = width // 2
    units = down_codes.shape[1]
    step = -(-half // 512) * 128
    cuts = tuple((c, min(step, half - c)) for c in range(0, half, step))
    dma = pltpu.SemaphoreType.DMA
    vmem = pltpu.VMEM
    in_vmem, anywhere = pl.BlockSpec(memory_space=vmem), pl.BlockSpec(memory_space=pl.ANY)
    return pl.pallas_call(
        functools.partial(layer_kernel, (tok, width, n_z, cuts)),
        out_shape=jax.ShapeDtypeStruct((tok, half), BF16),
        in_specs=[in_vmem] * 4 + [anywhere] + [in_vmem] * 2 + [anywhere] + [in_vmem] * 2,
        out_specs=in_vmem,
        scratch_shapes=[
            vmem(gate_up_codes.shape[1:], jnp.int32),
            vmem((down_codes.shape[2], units), jnp.int32),
            vmem((half // 64 * 8, units), jnp.int32),
            vmem(gate_up_scales.shape[1:], F32),
            vmem((2, half, 128), BF16),
            vmem((tok, half), F32),
            vmem((1, half), F32),
            vmem((ep_count * tok, width + SPARE), BF16),
            vmem((width + SPARE, gate_up_codes.shape[2]), BF16),
            vmem((2, half, units), BF16),
            vmem((2, ep_count * tok // 2, units), BF16),
            vmem((2, 2, 2, tok, half), BF16),
            vmem((2, 2, 2, tok, half), BF16),
            vmem((2, 2, tok, half), BF16),
            vmem((2, 2, tok, half), BF16),
            vmem((2, 2, 2, tok, half), BF16),
            vmem((3, tok, half), BF16),
            vmem((3, tok, half), BF16),
            dma((2,)),
            dma,
            dma,
            dma((2, n_z, CHUNKS)),
            dma((2, n_z, CHUNKS)),
            dma((2, n_z, CHUNKS)),
            dma((2, n_z, CHUNKS)),
            dma((2, n_z, CHUNKS, 2)),
            dma((2, n_z, CHUNKS, 2)),
            dma((2, 2, 4)),
            dma((2, 2, 4)),
            dma((2, 4)),
            dma((2, 4)),
            dma((3, 4)),
            dma((3, 4)),
        ],
        compiler_params=pltpu.CompilerParams(
            collective_id=0, has_side_effects=True, vmem_limit_bytes=63 * 1024 * 1024
        ),
    )(
        hidden,
        route_experts.T,
        route_weight.T,
        norm_gain.reshape(1, width),
        gate_up_codes[0],
        gate_up_scales[0],
        gate_up_bias,
        down_codes[0].T,
        down_scales[0],
        down_bias,
    )


def solution(mesh):
    def layer(*arrays):
        tok, top = arrays[1].shape
        ep_count, tp_count = lax.axis_size("ep"), lax.axis_size("tp")
        dense = 2 * top >= ep_count and tp_count == 2 and ep_count == 8 and tok == 64
        return (dense_shards if dense else shards)(*arrays)

    placed = (
        P(("groups", "ep"), None),
        P(("groups", "ep"), None),
        P(("groups", "ep"), None),
        P(),
        P("ep", None, "tp"),
        P("ep", None, "tp"),
        P("ep", "tp"),
        P("ep", "tp", None),
        P("ep", "tp", None),
        P("ep", "tp"),
    )
    return jax.shard_map(
        layer, mesh=mesh, in_specs=placed, out_specs=P(("groups", "ep"), "tp"), check_vma=False
    )
```

```python
import functools

import jax
import jax.numpy as jnp
from jax import lax
from jax.experimental import pallas as pl
from jax.experimental.pallas import tpu as pltpu
from jax.sharding import PartitionSpec as P

MAGNITUDES = 0xC8643210 - (1 << 32)
SPARE = 64


def decode_nibble(nibble):
    magnit = nibble & 7
    exponent = jnp.maximum(jnp.right_shift(magnit, 1) - 1, 0)
    doubled = jnp.where(magnit < 2, magnit, jnp.left_shift(2 + (magnit & 1), exponent))
    signed_val = doubled.astype(jnp.float32) * 0.5
    return jnp.where(nibble >= 8, -signed_val, signed_val)


def unpack_weights(packed, scaling):
    row_count = packed.shape[0]
    shifts = jnp.arange(8, dtype=jnp.int32) * 4
    nibble = jnp.right_shift(packed[:, :, None], shifts[None, None, :]) & 15
    nibble = nibble.reshape(row_count, packed.shape[1] * 8)
    signed_val = decode_nibble(nibble)
    signed_val = (
        signed_val.reshape(row_count // 32, 32, -1) * scaling.astype(jnp.float32)[:, None, :]
    )
    return signed_val.reshape(row_count, -1).astype(jnp.bfloat16)


def unpack_rows(packed, scaling):
    row_count = packed.shape[0] * 8
    shifts = jnp.arange(8, dtype=jnp.int32) * 4
    nibble = jnp.right_shift(packed[:, None, :], shifts[None, :, None]) & 15
    nibble = nibble.reshape(row_count, packed.shape[1])
    signed_val = decode_nibble(nibble)
    signed_val = (
        signed_val.reshape(row_count // 32, 32, -1) * scaling.astype(jnp.float32)[:, None, :]
    )
    return signed_val.reshape(row_count, -1).astype(jnp.bfloat16)


def rms_normed(hidden, norm_gain):
    widened = hidden.astype(jnp.float32)
    mean_square = jnp.mean(widened * widened, axis=-1, keepdims=True)
    scaled = widened * lax.rsqrt(mean_square + 1e-05) * norm_gain.astype(jnp.float32)
    return scaled.astype(jnp.bfloat16)


def shards(
    hidden,
    route_experts,
    route_weight,
    norm_gain,
    gate_up_codes,
    gate_up_scales,
    gate_up_bias,
    down_codes,
    down_scales,
    down_bias,
):
    ep_count = lax.axis_size("ep")
    tp_count = lax.axis_size("tp")
    tp_rank = lax.axis_index("tp")
    tok_count, model_width = hidden.shape
    top_count = route_experts.shape[1]
    capacity = min(tok_count, max(tp_count, 2 * tok_count * top_count // ep_count))
    normed = rms_normed(hidden, norm_gain)
    flat_routes = route_experts.reshape(-1)
    onehot = (flat_routes[:, None] == jnp.arange(ep_count, dtype=jnp.int32)[None, :]).astype(
        jnp.int32
    )
    before = jnp.cumsum(onehot, axis=0) - onehot
    slot_of = jnp.sum(before * onehot, axis=1)
    target = (flat_routes * capacity + slot_of).reshape(tok_count, top_count)
    columns = jnp.arange(ep_count * capacity, dtype=jnp.int32)
    matches = target[:, :, None] == columns[None, None, :]
    placing = jnp.any(matches, axis=1).astype(jnp.bfloat16)
    weighting = jnp.sum(jnp.where(matches, route_weight[:, :, None], 0.0), axis=1)
    outgoing = lax.dot_general(
        placing, normed, (((0,), (0,)), ((), ())), preferred_element_type=jnp.float32
    ).astype(jnp.bfloat16)
    outgoing = outgoing.reshape(ep_count, capacity, model_width)
    gate_up_weight = unpack_rows(gate_up_codes[0], gate_up_scales[0])
    down_weight = unpack_weights(down_codes[0], down_scales[0])
    arrived = lax.all_to_all(outgoing, "ep", split_axis=0, concat_axis=0, tiled=True)
    source_count, item_count, _ = arrived.shape
    flat_rows = arrived.reshape(source_count * item_count, model_width)
    projected = jnp.dot(
        flat_rows, gate_up_weight, preferred_element_type=jnp.float32
    ) + gate_up_bias[0].astype(jnp.float32)
    gate_part = jnp.minimum(projected[:, 0::2], 7.0)
    upward = jnp.clip(projected[:, 1::2], -7.0, 7.0)
    activated = (gate_part * jax.nn.sigmoid(1.702 * gate_part) * (upward + 1.0)).astype(
        jnp.bfloat16
    )
    partial_value = jnp.dot(activated, down_weight, preferred_element_type=jnp.float32)
    partial_value = partial_value.astype(jnp.bfloat16).astype(jnp.float32)
    partial_value = partial_value.reshape(source_count, item_count, model_width)
    summed = lax.psum_scatter(
        partial_value.astype(jnp.bfloat16), "tp", scatter_dimension=2, tiled=True
    ).astype(jnp.float32)
    answered = (summed + down_bias[0].astype(jnp.float32)).astype(jnp.bfloat16)
    came_back = lax.all_to_all(answered, "ep", split_axis=0, concat_axis=0, tiled=True)
    quarter = model_width // tp_count
    own_cols = lax.dynamic_slice_in_dim(hidden, tp_rank * quarter, quarter, 1).astype(jnp.float32)
    gathered = came_back.reshape(ep_count * capacity, quarter).astype(jnp.float32)
    layer_out = own_cols + jnp.dot(weighting, gathered, precision=lax.Precision.HIGHEST)
    return layer_out.astype(jnp.bfloat16)

BF16 = jnp.bfloat16
F32 = jnp.float32
CHUNKS = 2


def word_order(size, lone):
    pos = lax.broadcasted_iota(jnp.int32, (size, size), 1)
    col = lax.broadcasted_iota(jnp.int32, (size, size), 0)
    inner = pos & 63
    source = pos - inner + 8 * (inner & 7) + (inner >> 3)
    if lone:
        last = pos - (size - 32)
        half = size - 32 + 8 * (last & 3) + 2 * (last >> 3) + ((last & 7) >> 2)
        source = jnp.where(last >= 0, half, source)
    return (col == source).astype(F32).astype(BF16)


def matmul(a, b, contract=(1, 0)):
    return lax.dot_general(
        a, b, (((contract[0],), (contract[1],)), ((), ())), preferred_element_type=F32
    )


def column_blocks(total):
    blocks = [(start, 256) for start in range(0, total - total % 256, 256)]
    return blocks + ([(total // 256 * 256, total % 256)] if total % 256 else [])


def magnitude(words, quad):
    return (lax.shift_right_logical(jnp.full_like(words, MAGNITUDES), quad) & 15).astype(F32)


def decode_words(words, scales):
    pieces = []
    for quarter in range(4):
        j = 2 * quarter
        upper = words if j < 4 else lax.shift_right_logical(words, 16)
        pair = jnp.concatenate([upper, lax.shift_right_logical(words, 4 + j // 4 * 16)], axis=0)
        negative = (pair.astype(jnp.int16) & jnp.int16(8 << (4 * (j % 4)))) != 0
        sizes = []
        for i in (j, j + 1):
            moved = jnp.left_shift(words, 2) if i == 0 else lax.shift_right_logical(words, 4 * i - 2)
            sizes.append(magnitude(words, moved & 28))
        scale = scales[quarter]
        pieces.append(
            jnp.concatenate(sizes, axis=0).astype(BF16) * jnp.where(negative, -scale, scale)
        )
    return jnp.concatenate(pieces, axis=0)


def layer_kernel(
    sizes,
    hidden,
    routes,
    route_weights,
    gain,
    gate_codes_in,
    gate_scales_in,
    gate_bias,
    down_codes_in,
    down_scales_in,
    down_bias,
    out,
    gate_codes,
    down_codes,
    half_codes,
    gate_scales,
    down_scales,
    own_part,
    bias_part,
    rows_in,
    gate_weight,
    down_weight,
    activated,
    pair_out,
    pair_in,
    side_out,
    side_in,
    kept,
    step_out,
    step_in,
    load_sem,
    own_send,
    own_recv,
    line_send,
    line_recv,
    cross_send,
    cross_recv,
    pass_send,
    pass_recv,
    pair_send,
    pair_recv,
    side_send,
    side_recv,
    step_send,
    step_recv,
):
    tok, width, n_z, cuts = sizes
    half_rows = tok // 2
    part_rows = half_rows // CHUNKS
    half_cols = width // 2
    ep = lax.axis_index("ep")
    x = lax.axis_index("tp")
    z = ep // 2
    core = ep % 2
    partner = {"ep": 2 * z + 1 - core}
    across = {"tp": 1 - x}
    beside = z + 1 - 2 * (z % 2)
    beyond = (z + 2) % 4
    neighbour = {"ep": 2 * beside + core}
    opposite = {"ep": 2 * beyond + core}

    def copy(src, dst, send, recv, device):
        return pltpu.make_async_remote_copy(
            src_ref=src,
            dst_ref=dst,
            send_sem=send,
            recv_sem=recv,
            device_id=device,
            device_id_type=pl.DeviceIdType.MESH,
        )

    loads = [
        pltpu.make_async_copy(gate_codes_in, gate_codes, load_sem.at[0]),
        pltpu.make_async_copy(down_codes_in, down_codes, load_sem.at[1]),
    ]
    loads[0].start()
    barrier = pltpu.get_barrier_semaphore()
    others = [{"ep": 2 * ((z + d) % n_z) + core} for d in range(1, n_z)]
    for device in [partner, across] + others:
        pl.semaphore_signal(
            barrier, inc=1, device_id=device, device_id_type=pl.DeviceIdType.MESH
        )

    order = word_order(256, False)
    blocks = column_blocks(width)
    gain_row = gain[...].reshape(1, width)
    wide = jnp.concatenate(
        [matmul(hidden[:, c : c + n], order[:n, :n]) for c, n in blocks], axis=1
    )
    gain_row = jnp.concatenate(
        [matmul(gain_row[:, c : c + n], order[:n, :n]) for c, n in blocks], axis=1
    )
    plain = hidden[...].astype(F32)
    mean_square = jnp.mean(plain * plain, axis=-1, keepdims=True)
    normed = (wide * lax.rsqrt(mean_square + 1e-05) * gain_row).astype(BF16)
    number = lax.broadcasted_iota(jnp.int32, (SPARE, tok), 0)
    weight_at = jnp.zeros((SPARE, tok), F32)
    for k in range(routes.shape[0]):
        chosen = routes[k : k + 1, :] == number % (2 * n_z)
        weight_at = weight_at + jnp.where(chosen, route_weights[k : k + 1, :], 0.0)
    high = weight_at.astype(BF16).astype(F32)
    middle = (weight_at - high).astype(BF16).astype(F32)
    low = weight_at - high - middle
    piece = number // (2 * n_z)
    spare = jnp.where(
        piece == 0, high, jnp.where(piece == 1, middle, jnp.where(piece == 2, low, 0.0))
    )
    same = lax.broadcasted_iota(jnp.int32, (tok, tok), 0) == lax.broadcasted_iota(
        jnp.int32, (tok, tok), 1
    )
    spare_lanes = matmul(same.astype(F32).astype(BF16), spare.astype(BF16), (1, 1))
    aligned = width // 128 * 128
    mine = pl.ds(pl.multiple_of(ep * tok, tok), tok)
    rows_in[mine, :aligned] = normed[:, :aligned]
    rows_in[mine, aligned:] = jnp.concatenate(
        [normed[:, aligned:], spare_lanes.astype(BF16)], axis=1
    )

    pl.semaphore_wait(barrier, n_z + 1)

    def part(chip, half, k):
        start = (2 * chip + core) * tok + half * half_rows + k * part_rows
        return rows_in.at[pl.ds(pl.multiple_of(start, part_rows), part_rows)]

    near = 1 - z % 2

    def origin(side, s):
        return (z + n_z + (2 * side - 1) * s) % n_z

    def has(side, s):
        return side * (n_z - 1 - z) + (1 - side) * z >= s

    def goes(side):
        return side * z + (1 - side) * (n_z - 1 - z) >= 1

    def line_copy(side, s, k, chip):
        ref = part(chip, x, k)
        onward = {"ep": 2 * ((z + n_z + 1 - 2 * side) % n_z) + core}
        return copy(ref, ref, line_send.at[side, s, k], line_recv.at[side, s, k], onward)

    def cross_copy(side, s, k):
        ref = part(origin(side, s), x, k)
        return copy(ref, ref, cross_send.at[side, s, k], cross_recv.at[side, s, k], across)

    def pass_copy(side, s, k, i):
        ref = part(origin(side, s), x if i == 0 else 1 - x, k)
        return copy(ref, ref, pass_send.at[side, s, k, i], pass_recv.at[side, s, k, i], partner)

    def when(condition, action):
        pl.when(condition)(action)

    for k in range(CHUNKS):
        for side in range(2):
            when(goes(side), lambda: line_copy(side, 1, k, z).start())

    own_block = rows_in.at[mine]
    own = copy(own_block, own_block, own_send, own_recv, partner)
    own.start()

    def arrive(side, s, k):
        def action():
            line_copy(side, s, k, origin(side, s)).wait_recv()
            if s < n_z - 1:
                when(goes(side), lambda: line_copy(side, s + 1, k, origin(side, s)).start())
            pass_copy(side, s, k, 0).start()

        when(has(side, s), action)

    def cross(side, s, k):
        when(has(side, s), lambda: cross_copy(side, s, k).start())

    def arrive_crossed(side, s, k):
        def action():
            cross_copy(side, s, k).wait_recv()
            pass_copy(side, s, k, 1).start()

        when(has(side, s), action)

    def complete(side, s):
        def action():
            for k in range(CHUNKS):
                for i in range(2):
                    pass_copy(side, s, k, i).wait_recv()

        when(has(side, s), action)

    def drain(side, s):
        def action():
            for k in range(CHUNKS):
                cross_copy(side, s, k).wait_send()
                for i in range(2):
                    pass_copy(side, s, k, i).wait_send()
                if s < n_z - 1:
                    when(
                        goes(side),
                        lambda: line_copy(side, s + 1, k, origin(side, s)).wait_send(),
                    )

        when(has(side, s), action)

    far = 1 - near

    def first_arrives(k):
        arrive(near, 1, k)
        arrive(far, 1, k)
        cross(near, 1, k)

    def later_arrives(s, k):
        arrive(near, s, k)
        arrive(far, s, k)
        cross(near, s, k)
        cross(far, s, k)

    def crossed(s, k):
        arrive_crossed(near, s, k)
        arrive_crossed(far, s, k)

    gate_scales[...] = gate_scales_in[...].astype(F32) * 0.5
    gate_cols = gate_codes.shape[1]
    col_step = 512 if gate_cols % 512 == 0 else 256
    upper = lax.broadcasted_iota(jnp.int32, (16, col_step), 0) % 8 < 4

    def gate_rows(s, carry):
        base = pl.multiple_of(s * 8, 8)
        for col in range(0, gate_cols, col_step):
            words = gate_codes[pl.ds(base, 8), col : col + col_step]
            first, second = (
                jnp.broadcast_to(
                    gate_scales[pl.ds(2 * s + i, 1), col : col + col_step], (16, col_step)
                )
                for i in range(2)
            )
            scale = jnp.where(upper, first, second).astype(BF16)
            gate_weight[pl.ds(pl.multiple_of(s * 64, 64), 64), col : col + col_step] = (
                decode_words(words, [scale] * 4)
            )
        return carry

    gate_steps = gate_codes.shape[0] // 8
    gate_weight[pl.ds(width, SPARE), :] = jnp.zeros((SPARE, gate_cols), BF16)
    scale_rows = down_scales_in.shape[0]
    half_blocks = column_blocks(half_cols)
    tail_size = half_blocks[-1][1]
    tail_order = word_order(tail_size, True)
    for h in range(2):
        for c, n in half_blocks:
            picked = tail_order if n == tail_size else order
            block = down_scales_in[:, h * half_cols + c : h * half_cols + c + n]
            down_scales[h, c : c + n, :scale_rows] = matmul(picked, block, (0, 1)).astype(BF16)
    shown = jnp.where(x == 0, hidden[:, :half_cols], hidden[:, half_cols:])
    for c, n in half_blocks:
        picked = tail_order if n == tail_size else order
        own_part[:, c : c + n] = matmul(shown[:, c : c + n], picked)
        bias_part[:, c : c + n] = matmul(down_bias[:, c : c + n], picked)

    loads[0].wait()
    loads[1].start()
    marks = [0, gate_steps * 20 // 45, gate_steps * 30 // 45, gate_steps * 40 // 45]
    lax.fori_loop(marks[0], marks[1], gate_rows, 0)
    first_arrives(0)
    lax.fori_loop(marks[1], marks[2], gate_rows, 0)
    first_arrives(1)
    for k in range(CHUNKS):
        cross(far, 1, k)
    lax.fori_loop(marks[2], marks[3], gate_rows, 0)
    later_arrives(2, 0)
    lax.fori_loop(marks[3], gate_steps, gate_rows, 0)

    units = down_codes.shape[1]
    words_half = half_cols // 8
    down_steps = words_half // 8
    spread = (
        lax.broadcasted_iota(jnp.int32, (scale_rows, units), 1) // 32
        == lax.broadcasted_iota(jnp.int32, (scale_rows, units), 0)
    ).astype(F32) * 0.5
    spread = spread.astype(BF16)
    loads[1].wait()
    for h in range(2):
        half_codes[h, :words_half] = down_codes[h * words_half : (h + 1) * words_half, :]

    def down_rows(h, g, carry):
        base = pl.multiple_of(g * 128, 128)
        scale_block = down_scales[h, pl.ds(base, 128), :scale_rows]
        for col in range(0, units, 256):
            scale = matmul(scale_block, spread[:, col : col + 256]).astype(BF16)
            for i in range(2):
                words = half_codes[h, pl.ds(pl.multiple_of(g * 16 + 8 * i, 8), 8), col : col + 256]
                start = pl.multiple_of(base + 64 * i, 64)
                down_weight[h, pl.ds(start, 64), col : col + 256] = decode_words(
                    words, [scale[64 * i + 16 * j : 64 * i + 16 * j + 16] for j in range(4)]
                )
        return carry

    place = (lax.broadcasted_iota(jnp.int32, (8, units), 0) >> 2) * 4

    def down_last(h):
        base = down_steps * 64
        four = half_codes[h, down_steps * 8 : words_half, :]
        words = jnp.concatenate([four, four], axis=0)
        scale = matmul(down_scales[h, base : base + 32, :scale_rows], spread)
        pieces = []
        for i in range(4):
            shift = place + 8 * i
            quad = jnp.left_shift(lax.shift_right_logical(words, shift), 2) & 28
            negative = jnp.left_shift(words, 28 - shift) < 0
            part_scale = scale[8 * i : 8 * i + 8]
            pieces.append(magnitude(words, quad) * jnp.where(negative, -part_scale, part_scale))
        down_weight[h, base : base + 32, :] = jnp.concatenate(pieces, axis=0).astype(BF16)

    pair_steps = down_steps // 2
    middle_step = pair_steps // 2
    other_rows = functools.partial(down_rows, 1 - x)
    later_arrives(2, 1)
    lax.fori_loop(0, middle_step, other_rows, 0)
    for k in range(CHUNKS):
        arrive_crossed(near, 1, k)
    own_ahead = pair_steps // 4
    lax.fori_loop(0, own_ahead, functools.partial(down_rows, x), 0)

    picks = (
        lax.broadcasted_iota(jnp.int32, (256, 128), 0)
        == 2 * lax.broadcasted_iota(jnp.int32, (256, 128), 1)
    ).astype(F32).astype(BF16)
    batch_rows = 4 * tok
    group = z // 2
    place_in = z % 2
    starts = [
        pl.multiple_of(group * batch_rows, batch_rows),
        pl.multiple_of((1 - group) * batch_rows, batch_rows),
    ]

    def gate_tile(b, t, tile_cols, steps):
        for step in steps:
            step()
        cols = pl.ds(pl.multiple_of(t * tile_cols, tile_cols), tile_cols)
        projected = jnp.dot(
            rows_in[pl.ds(starts[b], batch_rows), :],
            gate_weight[:, cols],
            preferred_element_type=F32,
        ) + gate_bias[:, cols].astype(F32)
        gate_part = jnp.minimum(projected, 7.0)
        upward = pltpu.roll(jnp.clip(projected, -7.0, 7.0), tile_cols - 1, 1)
        value = (gate_part * jax.nn.sigmoid(1.702 * gate_part) * (upward + 1.0)).astype(BF16)
        for c in range(0, tile_cols, 256):
            at = pl.ds(pl.multiple_of(t * (tile_cols // 2) + c // 2, 128), 128)
            activated[b, :, at] = matmul(value[:, c : c + 256], picks).astype(BF16)

    def pair_copy(b, h, q):
        c, n = cuts[q]
        return copy(
            pair_out.at[b, h, :, :, pl.ds(c, n)],
            pair_in.at[b, h, :, :, pl.ds(c, n)],
            pair_send.at[b, h, q],
            pair_recv.at[b, h, q],
            partner,
        )

    def side_copy(b, q):
        c, n = cuts[q]
        return copy(
            side_out.at[b, :, :, pl.ds(c, n)],
            side_in.at[b, :, :, pl.ds(c, n)],
            side_send.at[b, q],
            side_recv.at[b, q],
            across,
        )

    def step_copy(i, q):
        c, n = cuts[q]
        return copy(
            step_out.at[i, :, pl.ds(c, n)],
            step_in.at[i, :, pl.ds(c, n)],
            step_send.at[i, q],
            step_recv.at[i, q],
            opposite if i == 2 else neighbour,
        )

    tail = lax.broadcasted_iota(jnp.int32, (batch_rows, SPARE), 1)

    def weights_of(b):
        extra = rows_in[pl.ds(starts[b], batch_rows), width:].astype(F32)
        hit = (tail == ep) | (tail == ep + 2 * n_z) | (tail == ep + 4 * n_z)
        return jnp.sum(jnp.where(hit, extra, 0.0), axis=1, keepdims=True)

    parts = range(len(cuts))

    def multiply(b, h, weight):
        which = 1 - x if h == 0 else x
        value = matmul(activated[b], down_weight[which], (1, 1))
        if h == 1:
            value = value + bias_part[...]
        value = value * weight
        for i in range(2):
            first = value[2 * i * tok : (2 * i + 1) * tok]
            second = value[(2 * i + 1) * tok : (2 * i + 2) * tok]
            pair_out[b, h, i] = jnp.where(core == 0, second, first).astype(BF16)
            kept[b, h, i] = jnp.where(core == 0, first, second).astype(BF16)
        for q in parts:
            pair_copy(b, h, q).start()

    def fold_pair(b, h, q):
        c, n = cuts[q]
        pair_copy(b, h, q).wait_recv()
        total = kept[b, h, :, :, c : c + n].astype(F32) + pair_in[
            b, h, :, :, c : c + n
        ].astype(F32)
        if h == 0:
            side_out[b, :, :, c : c + n] = total.astype(BF16)
            side_copy(b, q).start()
        else:
            kept[b, h, :, :, c : c + n] = total.astype(BF16)

    def folded(b, i, q):
        c, n = cuts[q]
        return kept[b, 1, i, :, c : c + n].astype(F32) + side_in[b, i, :, c : c + n].astype(F32)

    def fold_side(b, q):
        c, n = cuts[q]
        side_copy(b, q).wait_recv()
        step_out[b, :, c : c + n] = folded(b, 1 - place_in, q).astype(BF16)
        step_copy(b, q).start()
        if b == 0:
            own_part[:, c : c + n] = own_part[:, c : c + n] + folded(0, place_in, q)

    def fold_step(q):
        c, n = cuts[q]
        step_copy(1, q).wait_recv()
        total = folded(1, place_in, q) + step_in[1, :, c : c + n].astype(F32)
        step_out[2, :, c : c + n] = total.astype(BF16)
        step_copy(2, q).start()

    def add_step(i, q):
        c, n = cuts[q]
        step_copy(i, q).wait_recv()
        own_part[:, c : c + n] = own_part[:, c : c + n] + step_in[i, :, c : c + n].astype(F32)

    def write_out(q):
        c, n = cuts[q]
        at = c
        while at < c + n:
            left = half_cols - at
            size = tail_size if left == tail_size else min(256, c + n - at)
            if left > tail_size and left - size < tail_size:
                size = left - tail_size
            picked = tail_order if left == tail_size else order[:size, :size]
            block = own_part[:, at : at + size].astype(BF16)
            out[:, at : at + size] = matmul(block, picked, (1, 1)).astype(BF16)
            at += size

    half_tiles = gate_cols // 2

    def decode_steps(which, first, last):
        steps = [functools.partial(down_rows, which, g, 0) for g in range(first, last)]
        return steps + ([functools.partial(down_last, which)] if last == pair_steps else [])

    later_arrives(3, 0)
    own.wait_recv()
    complete(near, 1)
    near_weight = weights_of(0)
    mixed = 512
    tiles = gate_cols // mixed
    steps = decode_steps(1 - x, middle_step, pair_steps) + decode_steps(x, own_ahead, pair_steps)
    services = {
        0: [lambda: later_arrives(3, 1)],
        1: [lambda: arrive_crossed(far, 1, 0), lambda: arrive_crossed(far, 1, 1)],
        2: [lambda: crossed(2, 0)],
        3: [lambda: crossed(2, 1), lambda: crossed(3, 0)],
    }
    for t in range(tiles):
        cut = len(steps) * t // tiles, len(steps) * (t + 1) // tiles
        gate_tile(0, t, mixed, steps[cut[0] : cut[1]])
        for service in services.get(t, []):
            service()
    multiply(0, 0, near_weight)
    crossed(3, 1)
    multiply(0, 1, near_weight)
    for q in parts:
        fold_pair(0, 0, q)
    complete(far, 1)
    for s in range(2, n_z):
        complete(0, s)
        complete(1, s)
    far_weight = weights_of(1)
    gate_tile(1, 0, half_tiles, [])
    for q in parts:
        fold_pair(0, 1, q)
    gate_tile(1, 1, half_tiles, [])
    fold_side(0, 0)
    fold_side(0, 1)
    multiply(1, 0, far_weight)
    fold_side(0, 2)
    multiply(1, 1, far_weight)
    for q in parts:
        fold_pair(1, 0, q)
    fold_side(0, 3)
    for q in parts:
        fold_pair(1, 1, q)
    for q in parts:
        fold_side(1, q)
        if q:
            fold_step(q - 1)
    fold_step(len(cuts) - 1)
    for q in parts:
        add_step(0, q)
        add_step(2, q)
        write_out(q)

    own.wait_send()
    for side in range(2):

        def sent():
            for k in range(CHUNKS):
                line_copy(side, 1, k, z).wait_send()

        when(goes(side), sent)
        for s in range(1, n_z):
            drain(side, s)
    for q in parts:
        for b in range(2):
            for h in range(2):
                pair_copy(b, h, q).wait_send()
            side_copy(b, q).wait_send()
        for i in range(3):
            step_copy(i, q).wait_send()


def dense_shards(
    hidden,
    route_experts,
    route_weight,
    norm_gain,
    gate_up_codes,
    gate_up_scales,
    gate_up_bias,
    down_codes,
    down_scales,
    down_bias,
):
    ep_count = lax.axis_size("ep")
    tok, width = hidden.shape
    n_z = ep_count // 2
    half = width // 2
    units = down_codes.shape[1]
    last = half % 128 + 128
    step = -(-(half - last) // 384) * 128
    cuts = tuple((c, min(step, half - last - c)) for c in range(0, half - last, step))
    cuts += ((half - last, last),)
    dma = pltpu.SemaphoreType.DMA
    vmem = pltpu.VMEM
    in_vmem, anywhere = pl.BlockSpec(memory_space=vmem), pl.BlockSpec(memory_space=pl.ANY)
    return pl.pallas_call(
        functools.partial(layer_kernel, (tok, width, n_z, cuts)),
        out_shape=jax.ShapeDtypeStruct((tok, half), BF16),
        in_specs=[in_vmem] * 4 + [anywhere] + [in_vmem] * 2 + [anywhere] + [in_vmem] * 2,
        out_specs=in_vmem,
        scratch_shapes=[
            vmem(gate_up_codes.shape[1:], jnp.int32),
            vmem((down_codes.shape[2], units), jnp.int32),
            vmem((2, -(-half // 64) * 8, units), jnp.int32),
            vmem(gate_up_scales.shape[1:], F32),
            vmem((2, half, 128), BF16),
            vmem((tok, half), F32),
            vmem((1, half), F32),
            vmem((ep_count * tok, width + SPARE), BF16),
            vmem((width + SPARE, gate_up_codes.shape[2]), BF16),
            vmem((2, half, units), BF16),
            vmem((2, ep_count * tok // 2, units), BF16),
            vmem((2, 2, 2, tok, half), BF16),
            vmem((2, 2, 2, tok, half), BF16),
            vmem((2, 2, tok, half), BF16),
            vmem((2, 2, tok, half), BF16),
            vmem((2, 2, 2, tok, half), BF16),
            vmem((3, tok, half), BF16),
            vmem((3, tok, half), BF16),
            dma((2,)),
            dma,
            dma,
            dma((2, n_z, CHUNKS)),
            dma((2, n_z, CHUNKS)),
            dma((2, n_z, CHUNKS)),
            dma((2, n_z, CHUNKS)),
            dma((2, n_z, CHUNKS, 2)),
            dma((2, n_z, CHUNKS, 2)),
            dma((2, 2, 4)),
            dma((2, 2, 4)),
            dma((2, 4)),
            dma((2, 4)),
            dma((3, 4)),
            dma((3, 4)),
        ],
        compiler_params=pltpu.CompilerParams(
            collective_id=0, has_side_effects=True, vmem_limit_bytes=63 * 1024 * 1024
        ),
    )(
        hidden,
        route_experts.T,
        route_weight.T,
        norm_gain,
        gate_up_codes[0],
        gate_up_scales[0],
        gate_up_bias,
        down_codes[0].T,
        down_scales[0],
        down_bias,
    )


def solution(mesh):
    def layer(*arrays):
        tok, top = arrays[1].shape
        ep_count, tp_count = lax.axis_size("ep"), lax.axis_size("tp")
        dense = 2 * top >= ep_count and tp_count == 2 and ep_count == 8 and tok == 64
        return (dense_shards if dense else shards)(*arrays)

    placed = (
        P(("groups", "ep"), None),
        P(("groups", "ep"), None),
        P(("groups", "ep"), None),
        P(),
        P("ep", None, "tp"),
        P("ep", None, "tp"),
        P("ep", "tp"),
        P("ep", "tp", None),
        P("ep", "tp", None),
        P("ep", "tp"),
    )
    return jax.shard_map(
        layer, mesh=mesh, in_specs=placed, out_specs=P(("groups", "ep"), "tp"), check_vma=False
    )
```

```python
import functools

import jax
import jax.numpy as jnp
from jax import lax
from jax.experimental import pallas as pl
from jax.experimental.pallas import tpu as pltpu
from jax.sharding import PartitionSpec as P

MAGNITUDES = 0xC8643210 - (1 << 32)
SPARE = 64


def decode_nibble(nibble):
    magnit = nibble & 7
    exponent = jnp.maximum(jnp.right_shift(magnit, 1) - 1, 0)
    doubled = jnp.where(magnit < 2, magnit, jnp.left_shift(2 + (magnit & 1), exponent))
    signed_val = doubled.astype(jnp.float32) * 0.5
    return jnp.where(nibble >= 8, -signed_val, signed_val)


def unpack_weights(packed, scaling):
    row_count = packed.shape[0]
    shifts = jnp.arange(8, dtype=jnp.int32) * 4
    nibble = jnp.right_shift(packed[:, :, None], shifts[None, None, :]) & 15
    nibble = nibble.reshape(row_count, packed.shape[1] * 8)
    signed_val = decode_nibble(nibble)
    signed_val = (
        signed_val.reshape(row_count // 32, 32, -1) * scaling.astype(jnp.float32)[:, None, :]
    )
    return signed_val.reshape(row_count, -1).astype(jnp.bfloat16)


def unpack_rows(packed, scaling):
    row_count = packed.shape[0] * 8
    shifts = jnp.arange(8, dtype=jnp.int32) * 4
    nibble = jnp.right_shift(packed[:, None, :], shifts[None, :, None]) & 15
    nibble = nibble.reshape(row_count, packed.shape[1])
    signed_val = decode_nibble(nibble)
    signed_val = (
        signed_val.reshape(row_count // 32, 32, -1) * scaling.astype(jnp.float32)[:, None, :]
    )
    return signed_val.reshape(row_count, -1).astype(jnp.bfloat16)


def rms_normed(hidden, norm_gain):
    widened = hidden.astype(jnp.float32)
    mean_square = jnp.mean(widened * widened, axis=-1, keepdims=True)
    scaled = widened * lax.rsqrt(mean_square + 1e-05) * norm_gain.astype(jnp.float32)
    return scaled.astype(jnp.bfloat16)


def shards(
    hidden,
    route_experts,
    route_weight,
    norm_gain,
    gate_up_codes,
    gate_up_scales,
    gate_up_bias,
    down_codes,
    down_scales,
    down_bias,
):
    ep_count = lax.axis_size("ep")
    tp_count = lax.axis_size("tp")
    tp_rank = lax.axis_index("tp")
    tok_count, model_width = hidden.shape
    top_count = route_experts.shape[1]
    capacity = min(tok_count, max(tp_count, 2 * tok_count * top_count // ep_count))
    normed = rms_normed(hidden, norm_gain)
    flat_routes = route_experts.reshape(-1)
    onehot = (flat_routes[:, None] == jnp.arange(ep_count, dtype=jnp.int32)[None, :]).astype(
        jnp.int32
    )
    before = jnp.cumsum(onehot, axis=0) - onehot
    slot_of = jnp.sum(before * onehot, axis=1)
    target = (flat_routes * capacity + slot_of).reshape(tok_count, top_count)
    columns = jnp.arange(ep_count * capacity, dtype=jnp.int32)
    matches = target[:, :, None] == columns[None, None, :]
    placing = jnp.any(matches, axis=1).astype(jnp.bfloat16)
    weighting = jnp.sum(jnp.where(matches, route_weight[:, :, None], 0.0), axis=1)
    outgoing = lax.dot_general(
        placing, normed, (((0,), (0,)), ((), ())), preferred_element_type=jnp.float32
    ).astype(jnp.bfloat16)
    outgoing = outgoing.reshape(ep_count, capacity, model_width)
    gate_up_weight = unpack_rows(gate_up_codes[0], gate_up_scales[0])
    down_weight = unpack_weights(down_codes[0], down_scales[0])
    arrived = lax.all_to_all(outgoing, "ep", split_axis=0, concat_axis=0, tiled=True)
    source_count, item_count, _ = arrived.shape
    flat_rows = arrived.reshape(source_count * item_count, model_width)
    projected = jnp.dot(
        flat_rows, gate_up_weight, preferred_element_type=jnp.float32
    ) + gate_up_bias[0].astype(jnp.float32)
    gate_part = jnp.minimum(projected[:, 0::2], 7.0)
    upward = jnp.clip(projected[:, 1::2], -7.0, 7.0)
    activated = (gate_part * jax.nn.sigmoid(1.702 * gate_part) * (upward + 1.0)).astype(
        jnp.bfloat16
    )
    partial_value = jnp.dot(activated, down_weight, preferred_element_type=jnp.float32)
    partial_value = partial_value.astype(jnp.bfloat16).astype(jnp.float32)
    partial_value = partial_value.reshape(source_count, item_count, model_width)
    summed = lax.psum_scatter(
        partial_value.astype(jnp.bfloat16), "tp", scatter_dimension=2, tiled=True
    ).astype(jnp.float32)
    answered = (summed + down_bias[0].astype(jnp.float32)).astype(jnp.bfloat16)
    came_back = lax.all_to_all(answered, "ep", split_axis=0, concat_axis=0, tiled=True)
    quarter = model_width // tp_count
    own_cols = lax.dynamic_slice_in_dim(hidden, tp_rank * quarter, quarter, 1).astype(jnp.float32)
    gathered = came_back.reshape(ep_count * capacity, quarter).astype(jnp.float32)
    layer_out = own_cols + jnp.dot(weighting, gathered, precision=lax.Precision.HIGHEST)
    return layer_out.astype(jnp.bfloat16)

BF16 = jnp.bfloat16
F32 = jnp.float32
CHUNKS = 2


def word_order(size, lone):
    pos = lax.broadcasted_iota(jnp.int32, (size, size), 1)
    col = lax.broadcasted_iota(jnp.int32, (size, size), 0)
    inner = pos & 63
    source = pos - inner + 8 * (inner & 7) + (inner >> 3)
    if lone:
        last = pos - (size - 32)
        half = size - 32 + 8 * (last & 3) + 2 * (last >> 3) + ((last & 7) >> 2)
        source = jnp.where(last >= 0, half, source)
    return (col == source).astype(F32).astype(BF16)


def matmul(a, b, contract=(1, 0)):
    return lax.dot_general(
        a, b, (((contract[0],), (contract[1],)), ((), ())), preferred_element_type=F32
    )


def column_blocks(total):
    blocks = [(start, 256) for start in range(0, total - total % 256, 256)]
    return blocks + ([(total // 256 * 256, total % 256)] if total % 256 else [])


def magnitude(words, quad):
    return (lax.shift_right_logical(jnp.full_like(words, MAGNITUDES), quad) & 15).astype(F32)


def decode_words(words, scales):
    pieces = []
    for quarter in range(4):
        j = 2 * quarter
        upper = words if j < 4 else lax.shift_right_logical(words, 16)
        pair = jnp.concatenate([upper, lax.shift_right_logical(words, 4 + j // 4 * 16)], axis=0)
        negative = (pair.astype(jnp.int16) & jnp.int16(8 << (4 * (j % 4)))) != 0
        sizes = []
        for i in (j, j + 1):
            moved = jnp.left_shift(words, 2) if i == 0 else lax.shift_right_logical(words, 4 * i - 2)
            sizes.append(magnitude(words, moved & 28))
        scale = scales[quarter]
        pieces.append(
            jnp.concatenate(sizes, axis=0).astype(BF16) * jnp.where(negative, -scale, scale)
        )
    return jnp.concatenate(pieces, axis=0)


def layer_kernel(
    sizes,
    hidden,
    routes,
    route_weights,
    gain,
    gate_codes_in,
    gate_scales_in,
    gate_bias,
    down_codes_in,
    down_scales_in,
    down_bias,
    out,
    gate_codes,
    down_codes,
    half_codes,
    gate_scales,
    down_scales,
    own_part,
    bias_part,
    rows_in,
    gate_weight,
    down_weight,
    activated,
    pair_out,
    pair_in,
    side_out,
    side_in,
    kept,
    step_out,
    step_in,
    load_sem,
    own_send,
    own_recv,
    line_send,
    line_recv,
    cross_send,
    cross_recv,
    pass_send,
    pass_recv,
    pair_send,
    pair_recv,
    side_send,
    side_recv,
    step_send,
    step_recv,
):
    tok, width, n_z, cuts = sizes
    half_rows = tok // 2
    part_rows = half_rows // CHUNKS
    half_cols = width // 2
    ep = lax.axis_index("ep")
    x = lax.axis_index("tp")
    z = ep // 2
    core = ep % 2
    partner = {"ep": 2 * z + 1 - core}
    across = {"tp": 1 - x}
    beside = z + 1 - 2 * (z % 2)
    beyond = (z + 2) % 4
    neighbour = {"ep": 2 * beside + core}
    opposite = {"ep": 2 * beyond + core}

    def copy(src, dst, send, recv, device):
        return pltpu.make_async_remote_copy(
            src_ref=src,
            dst_ref=dst,
            send_sem=send,
            recv_sem=recv,
            device_id=device,
            device_id_type=pl.DeviceIdType.MESH,
        )

    loads = [
        pltpu.make_async_copy(gate_codes_in, gate_codes, load_sem.at[0]),
        pltpu.make_async_copy(down_codes_in, down_codes, load_sem.at[1]),
    ]
    loads[0].start()
    barrier = pltpu.get_barrier_semaphore()
    others = [{"ep": 2 * ((z + d) % n_z) + core} for d in range(1, n_z)]
    for device in [partner, across] + others:
        pl.semaphore_signal(
            barrier, inc=1, device_id=device, device_id_type=pl.DeviceIdType.MESH
        )

    order = word_order(256, False)
    blocks = column_blocks(width)
    gain_row = gain[...].reshape(1, width)
    wide = jnp.concatenate(
        [matmul(hidden[:, c : c + n], order[:n, :n]) for c, n in blocks], axis=1
    )
    gain_row = jnp.concatenate(
        [matmul(gain_row[:, c : c + n], order[:n, :n]) for c, n in blocks], axis=1
    )
    plain = hidden[...].astype(F32)
    mean_square = jnp.mean(plain * plain, axis=-1, keepdims=True)
    normed = (wide * lax.rsqrt(mean_square + 1e-05) * gain_row).astype(BF16)
    number = lax.broadcasted_iota(jnp.int32, (SPARE, tok), 0)
    weight_at = jnp.zeros((SPARE, tok), F32)
    for k in range(routes.shape[0]):
        chosen = routes[k : k + 1, :] == number % (2 * n_z)
        weight_at = weight_at + jnp.where(chosen, route_weights[k : k + 1, :], 0.0)
    high = weight_at.astype(BF16).astype(F32)
    middle = (weight_at - high).astype(BF16).astype(F32)
    low = weight_at - high - middle
    piece = number // (2 * n_z)
    spare = jnp.where(
        piece == 0, high, jnp.where(piece == 1, middle, jnp.where(piece == 2, low, 0.0))
    )
    same = lax.broadcasted_iota(jnp.int32, (tok, tok), 0) == lax.broadcasted_iota(
        jnp.int32, (tok, tok), 1
    )
    spare_lanes = matmul(same.astype(F32).astype(BF16), spare.astype(BF16), (1, 1))
    aligned = width // 128 * 128
    mine = pl.ds(pl.multiple_of(ep * tok, tok), tok)
    rows_in[mine, :aligned] = normed[:, :aligned]
    rows_in[mine, aligned:] = jnp.concatenate(
        [normed[:, aligned:], spare_lanes.astype(BF16)], axis=1
    )

    pl.semaphore_wait(barrier, n_z + 1)

    def part(chip, half, k):
        start = (2 * chip + core) * tok + half * half_rows + k * part_rows
        return rows_in.at[pl.ds(pl.multiple_of(start, part_rows), part_rows)]

    near = 1 - z % 2

    def origin(side, s):
        return (z + n_z + (2 * side - 1) * s) % n_z

    def has(side, s):
        return side * (n_z - 1 - z) + (1 - side) * z >= s

    def goes(side):
        return side * z + (1 - side) * (n_z - 1 - z) >= 1

    def line_copy(side, s, k, chip):
        ref = part(chip, x, k)
        onward = {"ep": 2 * ((z + n_z + 1 - 2 * side) % n_z) + core}
        return copy(ref, ref, line_send.at[side, s, k], line_recv.at[side, s, k], onward)

    def cross_copy(side, s, k):
        ref = part(origin(side, s), x, k)
        return copy(ref, ref, cross_send.at[side, s, k], cross_recv.at[side, s, k], across)

    def pass_copy(side, s, k, i):
        ref = part(origin(side, s), x if i == 0 else 1 - x, k)
        return copy(ref, ref, pass_send.at[side, s, k, i], pass_recv.at[side, s, k, i], partner)

    def when(condition, action):
        pl.when(condition)(action)

    for k in range(CHUNKS):
        for side in range(2):
            when(goes(side), lambda: line_copy(side, 1, k, z).start())

    own_block = rows_in.at[mine]
    own = copy(own_block, own_block, own_send, own_recv, partner)
    own.start()

    def arrive(side, s, k):
        def action():
            line_copy(side, s, k, origin(side, s)).wait_recv()
            if s < n_z - 1:
                when(goes(side), lambda: line_copy(side, s + 1, k, origin(side, s)).start())
            pass_copy(side, s, k, 0).start()

        when(has(side, s), action)

    def cross(side, s, k):
        when(has(side, s), lambda: cross_copy(side, s, k).start())

    def arrive_crossed(side, s, k):
        def action():
            cross_copy(side, s, k).wait_recv()
            pass_copy(side, s, k, 1).start()

        when(has(side, s), action)

    def complete(side, s):
        def action():
            for k in range(CHUNKS):
                for i in range(2):
                    pass_copy(side, s, k, i).wait_recv()

        when(has(side, s), action)

    def drain(side, s):
        def action():
            for k in range(CHUNKS):
                cross_copy(side, s, k).wait_send()
                for i in range(2):
                    pass_copy(side, s, k, i).wait_send()
                if s < n_z - 1:
                    when(
                        goes(side),
                        lambda: line_copy(side, s + 1, k, origin(side, s)).wait_send(),
                    )

        when(has(side, s), action)

    far = 1 - near

    def first_arrives(k):
        arrive(near, 1, k)
        arrive(far, 1, k)
        cross(near, 1, k)

    def later_arrives(s, k):
        arrive(near, s, k)
        arrive(far, s, k)
        cross(near, s, k)
        cross(far, s, k)

    def crossed(s, k):
        arrive_crossed(near, s, k)
        arrive_crossed(far, s, k)

    gate_scales[...] = gate_scales_in[...].astype(F32) * 0.5
    gate_cols = gate_codes.shape[1]
    col_step = 512 if gate_cols % 512 == 0 else 256
    upper = lax.broadcasted_iota(jnp.int32, (16, col_step), 0) % 8 < 4

    def gate_rows(s, carry):
        base = pl.multiple_of(s * 8, 8)
        for col in range(0, gate_cols, col_step):
            words = gate_codes[pl.ds(base, 8), col : col + col_step]
            first, second = (
                jnp.broadcast_to(
                    gate_scales[pl.ds(2 * s + i, 1), col : col + col_step], (16, col_step)
                )
                for i in range(2)
            )
            scale = jnp.where(upper, first, second).astype(BF16)
            gate_weight[pl.ds(pl.multiple_of(s * 64, 64), 64), col : col + col_step] = (
                decode_words(words, [scale] * 4)
            )
        return carry

    gate_steps = gate_codes.shape[0] // 8
    gate_weight[pl.ds(width, SPARE), :] = jnp.zeros((SPARE, gate_cols), BF16)
    scale_rows = down_scales_in.shape[0]
    half_blocks = column_blocks(half_cols)
    tail_size = half_blocks[-1][1]
    tail_order = word_order(tail_size, True)
    for h in range(2):
        for c, n in half_blocks:
            picked = tail_order if n == tail_size else order
            block = down_scales_in[:, h * half_cols + c : h * half_cols + c + n]
            down_scales[h, c : c + n, :scale_rows] = matmul(picked, block, (0, 1)).astype(BF16)
    shown = jnp.where(x == 0, hidden[:, :half_cols], hidden[:, half_cols:])
    for c, n in half_blocks:
        picked = tail_order if n == tail_size else order
        own_part[:, c : c + n] = matmul(shown[:, c : c + n], picked)
        bias_part[:, c : c + n] = matmul(down_bias[:, c : c + n], picked)

    loads[0].wait()
    loads[1].start()
    marks = [0, gate_steps * 20 // 45, gate_steps * 30 // 45, gate_steps * 40 // 45]
    lax.fori_loop(marks[0], marks[1], gate_rows, 0)
    first_arrives(0)
    lax.fori_loop(marks[1], marks[2], gate_rows, 0)
    first_arrives(1)
    for k in range(CHUNKS):
        cross(far, 1, k)
    lax.fori_loop(marks[2], marks[3], gate_rows, 0)
    later_arrives(2, 0)
    lax.fori_loop(marks[3], gate_steps, gate_rows, 0)

    units = down_codes.shape[1]
    words_half = half_cols // 8
    down_steps = words_half // 8
    spread = (
        lax.broadcasted_iota(jnp.int32, (scale_rows, units), 1) // 32
        == lax.broadcasted_iota(jnp.int32, (scale_rows, units), 0)
    ).astype(F32) * 0.5
    spread = spread.astype(BF16)
    loads[1].wait()
    for h in range(2):
        half_codes[h, :words_half] = down_codes[h * words_half : (h + 1) * words_half, :]

    def down_rows(h, g, carry):
        base = pl.multiple_of(g * 128, 128)
        scale_block = down_scales[h, pl.ds(base, 128), :scale_rows]
        for col in range(0, units, 256):
            scale = matmul(scale_block, spread[:, col : col + 256]).astype(BF16)
            for i in range(2):
                words = half_codes[h, pl.ds(pl.multiple_of(g * 16 + 8 * i, 8), 8), col : col + 256]
                start = pl.multiple_of(base + 64 * i, 64)
                down_weight[h, pl.ds(start, 64), col : col + 256] = decode_words(
                    words, [scale[64 * i + 16 * j : 64 * i + 16 * j + 16] for j in range(4)]
                )
        return carry

    place = (lax.broadcasted_iota(jnp.int32, (8, units), 0) >> 2) * 4

    def down_last(h):
        base = down_steps * 64
        four = half_codes[h, down_steps * 8 : words_half, :]
        words = jnp.concatenate([four, four], axis=0)
        scale = matmul(down_scales[h, base : base + 32, :scale_rows], spread)
        pieces = []
        for i in range(4):
            shift = place + 8 * i
            quad = jnp.left_shift(lax.shift_right_logical(words, shift), 2) & 28
            negative = jnp.left_shift(words, 28 - shift) < 0
            part_scale = scale[8 * i : 8 * i + 8]
            pieces.append(magnitude(words, quad) * jnp.where(negative, -part_scale, part_scale))
        down_weight[h, base : base + 32, :] = jnp.concatenate(pieces, axis=0).astype(BF16)

    pair_steps = down_steps // 2
    middle_step = pair_steps // 2
    other_rows = functools.partial(down_rows, 1 - x)
    later_arrives(2, 1)
    lax.fori_loop(0, middle_step, other_rows, 0)
    for k in range(CHUNKS):
        arrive_crossed(near, 1, k)
    own_ahead = pair_steps // 4
    lax.fori_loop(0, own_ahead, functools.partial(down_rows, x), 0)

    picks = (
        lax.broadcasted_iota(jnp.int32, (256, 128), 0)
        == 2 * lax.broadcasted_iota(jnp.int32, (256, 128), 1)
    ).astype(F32).astype(BF16)
    batch_rows = 4 * tok
    group = z // 2
    place_in = z % 2
    starts = [
        pl.multiple_of(group * batch_rows, batch_rows),
        pl.multiple_of((1 - group) * batch_rows, batch_rows),
    ]

    def gate_tile(b, t, tile_cols, steps):
        for step in steps:
            step()
        cols = pl.ds(pl.multiple_of(t * tile_cols, tile_cols), tile_cols)
        projected = jnp.dot(
            rows_in[pl.ds(starts[b], batch_rows), :],
            gate_weight[:, cols],
            preferred_element_type=F32,
        ) + gate_bias[:, cols].astype(F32)
        gate_part = jnp.minimum(projected, 7.0)
        upward = pltpu.roll(jnp.clip(projected, -7.0, 7.0), tile_cols - 1, 1)
        value = (gate_part * jax.nn.sigmoid(1.702 * gate_part) * (upward + 1.0)).astype(BF16)
        for c in range(0, tile_cols, 256):
            at = pl.ds(pl.multiple_of(t * (tile_cols // 2) + c // 2, 128), 128)
            activated[b, :, at] = matmul(value[:, c : c + 256], picks).astype(BF16)

    def pair_copy(b, h, q):
        c, n = cuts[q]
        return copy(
            pair_out.at[b, h, :, :, pl.ds(c, n)],
            pair_in.at[b, h, :, :, pl.ds(c, n)],
            pair_send.at[b, h, q],
            pair_recv.at[b, h, q],
            partner,
        )

    def side_copy(b, i, q):
        c, n = cuts[q]
        return copy(
            side_out.at[b, i, :, pl.ds(c, n)],
            side_in.at[b, i, :, pl.ds(c, n)],
            side_send.at[b, i, q],
            side_recv.at[b, i, q],
            across,
        )

    def step_copy(i, q):
        c, n = cuts[q]
        return copy(
            step_out.at[i, :, pl.ds(c, n)],
            step_in.at[i, :, pl.ds(c, n)],
            step_send.at[i, q],
            step_recv.at[i, q],
            opposite if i == 2 else neighbour,
        )

    tail = lax.broadcasted_iota(jnp.int32, (batch_rows, SPARE), 1)

    def weights_of(b):
        extra = rows_in[pl.ds(starts[b], batch_rows), width:].astype(F32)
        hit = (tail == ep) | (tail == ep + 2 * n_z) | (tail == ep + 4 * n_z)
        return jnp.sum(jnp.where(hit, extra, 0.0), axis=1, keepdims=True)

    parts = range(len(cuts))

    def multiply(b, h, weight):
        which = 1 - x if h == 0 else x
        value = matmul(activated[b], down_weight[which], (1, 1))
        if h == 1:
            value = value + bias_part[...]
        value = value * weight
        for i in range(2):
            first = value[2 * i * tok : (2 * i + 1) * tok]
            second = value[(2 * i + 1) * tok : (2 * i + 2) * tok]
            pair_out[b, h, i] = jnp.where(core == 0, second, first).astype(BF16)
            kept[b, h, i] = jnp.where(core == 0, first, second).astype(BF16)
        for q in parts:
            pair_copy(b, h, q).start()

    def fold_pair(b, h, q):
        c, n = cuts[q]
        pair_copy(b, h, q).wait_recv()
        total = kept[b, h, :, :, c : c + n].astype(F32) + pair_in[
            b, h, :, :, c : c + n
        ].astype(F32)
        if h == 0:
            side_out[b, :, :, c : c + n] = total.astype(BF16)
        else:
            kept[b, h, :, :, c : c + n] = total.astype(BF16)

    def folded(b, i, q):
        c, n = cuts[q]
        side_copy(b, i, q).wait_recv()
        return kept[b, 1, i, :, c : c + n].astype(F32) + side_in[b, i, :, c : c + n].astype(F32)

    def fold_side(b, q):
        c, n = cuts[q]
        step_out[b, :, c : c + n] = folded(b, 1 - place_in, q).astype(BF16)
        step_copy(b, q).start()

    def fold_step(q):
        c, n = cuts[q]
        total = folded(1, place_in, q)
        step_copy(1, q).wait_recv()
        total = total + step_in[1, :, c : c + n].astype(F32)
        step_out[2, :, c : c + n] = total.astype(BF16)
        step_copy(2, q).start()

    def fold_own(q):
        c, n = cuts[q]
        total = own_part[:, c : c + n]
        for i in (0, 2):
            step_copy(i, q).wait_recv()
            total = total + step_in[i, :, c : c + n].astype(F32)
        own_part[:, c : c + n] = total + folded(0, place_in, q)

    def write_out(q):
        c, n = cuts[q]
        at = c
        while at < c + n:
            left = half_cols - at
            size = tail_size if left == tail_size else min(256, c + n - at)
            if left > tail_size and left - size < tail_size:
                size = left - tail_size
            picked = tail_order if left == tail_size else order[:size, :size]
            block = own_part[:, at : at + size].astype(BF16)
            out[:, at : at + size] = matmul(block, picked, (1, 1)).astype(BF16)
            at += size


    def decode_steps(which, first, last):
        steps = [functools.partial(down_rows, which, g, 0) for g in range(first, last)]
        return steps + ([functools.partial(down_last, which)] if last == pair_steps else [])

    later_arrives(3, 0)
    own.wait_recv()
    complete(near, 1)
    near_weight = weights_of(0)
    mixed = 512
    tiles = gate_cols // mixed
    steps = decode_steps(1 - x, middle_step, pair_steps) + decode_steps(x, own_ahead, pair_steps)
    services = {
        0: [lambda: later_arrives(3, 1)],
        1: [lambda: arrive_crossed(far, 1, 0), lambda: arrive_crossed(far, 1, 1)],
        2: [lambda: crossed(2, 0)],
        3: [lambda: crossed(2, 1), lambda: crossed(3, 0), lambda: crossed(3, 1)],
    }
    for t in range(tiles):
        cut = len(steps) * t // tiles, len(steps) * (t + 1) // tiles
        gate_tile(0, t, mixed, steps[cut[0] : cut[1]])
        for service in services.get(t, []):
            service()
    complete(far, 1)
    for s in range(2, n_z):
        complete(0, s)
        complete(1, s)
    far_weight = weights_of(1)
    gate_tile(1, 0, gate_cols, [])
    multiply(1, 0, far_weight)
    multiply(1, 1, far_weight)

    def send(b, which, q):
        for i in which:
            side_copy(b, i, q).start()

    def sent(b, which, q):
        for i in which:
            side_copy(b, i, q).wait_send()

    theirs, ours = (1 - place_in,), (place_in,)
    for q in parts:
        fold_pair(1, 0, q)
        if q < 2:
            send(1, (0, 1), q)
    multiply(0, 0, near_weight)
    multiply(0, 1, near_weight)
    sent(1, (0, 1), 0)
    send(1, (0, 1), 2)
    for q in parts:
        fold_pair(1, 1, q)
    for q in parts:
        fold_pair(0, 0, q)
    for q in parts:
        fold_pair(0, 1, q)
    fold_side(1, 0)
    sent(1, (0, 1), 1)
    send(1, (0, 1), 3)
    fold_side(1, 1)
    sent(1, (0, 1), 2)
    send(0, theirs, 0)
    send(0, theirs, 1)
    fold_step(0)
    fold_side(1, 2)
    sent(1, (0, 1), 3)
    send(0, theirs, 2)
    send(0, theirs, 3)
    fold_step(1)
    fold_side(1, 3)
    for q in (0, 1):
        sent(0, theirs, q)
        send(0, ours, q)
    fold_step(2)
    for q in (0, 1):
        fold_side(0, q)
    for q in (2, 3):
        sent(0, theirs, q)
        send(0, ours, q)
    fold_step(3)
    for q in (2, 3):
        fold_side(0, q)
    for q in parts:
        fold_own(q)
        write_out(q)

    own.wait_send()
    for side in range(2):

        def sent():
            for k in range(CHUNKS):
                line_copy(side, 1, k, z).wait_send()

        when(goes(side), sent)
        for s in range(1, n_z):
            drain(side, s)
    for q in parts:
        for b in range(2):
            for h in range(2):
                pair_copy(b, h, q).wait_send()
        side_copy(0, place_in, q).wait_send()
        for i in range(3):
            step_copy(i, q).wait_send()


def dense_shards(
    hidden,
    route_experts,
    route_weight,
    norm_gain,
    gate_up_codes,
    gate_up_scales,
    gate_up_bias,
    down_codes,
    down_scales,
    down_bias,
):
    ep_count = lax.axis_size("ep")
    tok, width = hidden.shape
    n_z = ep_count // 2
    half = width // 2
    units = down_codes.shape[1]
    step = -(-half // 512) * 128
    edges = [0] + [step * i - 128 for i in range(1, 4)] + [half]
    cuts = tuple((low, high - low) for low, high in zip(edges[:-1], edges[1:]))
    dma = pltpu.SemaphoreType.DMA
    vmem = pltpu.VMEM
    in_vmem, anywhere = pl.BlockSpec(memory_space=vmem), pl.BlockSpec(memory_space=pl.ANY)
    return pl.pallas_call(
        functools.partial(layer_kernel, (tok, width, n_z, cuts)),
        out_shape=jax.ShapeDtypeStruct((tok, half), BF16),
        in_specs=[in_vmem] * 4 + [anywhere] + [in_vmem] * 2 + [anywhere] + [in_vmem] * 2,
        out_specs=in_vmem,
        scratch_shapes=[
            vmem(gate_up_codes.shape[1:], jnp.int32),
            vmem((down_codes.shape[2], units), jnp.int32),
            vmem((2, -(-half // 64) * 8, units), jnp.int32),
            vmem(gate_up_scales.shape[1:], F32),
            vmem((2, half, 128), BF16),
            vmem((tok, half), F32),
            vmem((1, half), F32),
            vmem((ep_count * tok, width + SPARE), BF16),
            vmem((width + SPARE, gate_up_codes.shape[2]), BF16),
            vmem((2, half, units), BF16),
            vmem((2, ep_count * tok // 2, units), BF16),
            vmem((2, 2, 2, tok, half), BF16),
            vmem((2, 2, 2, tok, half), BF16),
            vmem((2, 2, tok, half), BF16),
            vmem((2, 2, tok, half), BF16),
            vmem((2, 2, 2, tok, half), BF16),
            vmem((3, tok, half), BF16),
            vmem((3, tok, half), BF16),
            dma((2,)),
            dma,
            dma,
            dma((2, n_z, CHUNKS)),
            dma((2, n_z, CHUNKS)),
            dma((2, n_z, CHUNKS)),
            dma((2, n_z, CHUNKS)),
            dma((2, n_z, CHUNKS, 2)),
            dma((2, n_z, CHUNKS, 2)),
            dma((2, 2, 4)),
            dma((2, 2, 4)),
            dma((2, 2, 4)),
            dma((2, 2, 4)),
            dma((3, 4)),
            dma((3, 4)),
        ],
        compiler_params=pltpu.CompilerParams(
            collective_id=0, has_side_effects=True, vmem_limit_bytes=63 * 1024 * 1024
        ),
    )(
        hidden,
        route_experts.T,
        route_weight.T,
        norm_gain,
        gate_up_codes[0],
        gate_up_scales[0],
        gate_up_bias,
        down_codes[0].T,
        down_scales[0],
        down_bias,
    )


def solution(mesh):
    def layer(*arrays):
        tok, top = arrays[1].shape
        ep_count, tp_count = lax.axis_size("ep"), lax.axis_size("tp")
        dense = 2 * top >= ep_count and tp_count == 2 and ep_count == 8 and tok == 64
        return (dense_shards if dense else shards)(*arrays)

    placed = (
        P(("groups", "ep"), None),
        P(("groups", "ep"), None),
        P(("groups", "ep"), None),
        P(),
        P("ep", None, "tp"),
        P("ep", None, "tp"),
        P("ep", "tp"),
        P("ep", "tp", None),
        P("ep", "tp", None),
        P("ep", "tp"),
    )
    return jax.shard_map(
        layer, mesh=mesh, in_specs=placed, out_specs=P(("groups", "ep"), "tp"), check_vma=False
    )
```

```python
import functools

import jax
import jax.numpy as jnp
from jax import lax
from jax.experimental import pallas as pl
from jax.experimental.pallas import tpu as pltpu
from jax.sharding import PartitionSpec as P

MAGNITUDES = 0xC8643210 - (1 << 32)
SPARE = 64


def decode_nibble(nibble):
    magnit = nibble & 7
    exponent = jnp.maximum(jnp.right_shift(magnit, 1) - 1, 0)
    doubled = jnp.where(magnit < 2, magnit, jnp.left_shift(2 + (magnit & 1), exponent))
    signed_val = doubled.astype(jnp.float32) * 0.5
    return jnp.where(nibble >= 8, -signed_val, signed_val)


def unpack_weights(packed, scaling):
    row_count = packed.shape[0]
    shifts = jnp.arange(8, dtype=jnp.int32) * 4
    nibble = jnp.right_shift(packed[:, :, None], shifts[None, None, :]) & 15
    nibble = nibble.reshape(row_count, packed.shape[1] * 8)
    signed_val = decode_nibble(nibble)
    signed_val = (
        signed_val.reshape(row_count // 32, 32, -1) * scaling.astype(jnp.float32)[:, None, :]
    )
    return signed_val.reshape(row_count, -1).astype(jnp.bfloat16)


def unpack_rows(packed, scaling):
    row_count = packed.shape[0] * 8
    shifts = jnp.arange(8, dtype=jnp.int32) * 4
    nibble = jnp.right_shift(packed[:, None, :], shifts[None, :, None]) & 15
    nibble = nibble.reshape(row_count, packed.shape[1])
    signed_val = decode_nibble(nibble)
    signed_val = (
        signed_val.reshape(row_count // 32, 32, -1) * scaling.astype(jnp.float32)[:, None, :]
    )
    return signed_val.reshape(row_count, -1).astype(jnp.bfloat16)


def rms_normed(hidden, norm_gain):
    widened = hidden.astype(jnp.float32)
    mean_square = jnp.mean(widened * widened, axis=-1, keepdims=True)
    scaled = widened * lax.rsqrt(mean_square + 1e-05) * norm_gain.astype(jnp.float32)
    return scaled.astype(jnp.bfloat16)


def shards(
    hidden,
    route_experts,
    route_weight,
    norm_gain,
    gate_up_codes,
    gate_up_scales,
    gate_up_bias,
    down_codes,
    down_scales,
    down_bias,
):
    ep_count = lax.axis_size("ep")
    tp_count = lax.axis_size("tp")
    tp_rank = lax.axis_index("tp")
    tok_count, model_width = hidden.shape
    top_count = route_experts.shape[1]
    capacity = min(tok_count, max(tp_count, 2 * tok_count * top_count // ep_count))
    normed = rms_normed(hidden, norm_gain)
    flat_routes = route_experts.reshape(-1)
    onehot = (flat_routes[:, None] == jnp.arange(ep_count, dtype=jnp.int32)[None, :]).astype(
        jnp.int32
    )
    before = jnp.cumsum(onehot, axis=0) - onehot
    slot_of = jnp.sum(before * onehot, axis=1)
    target = (flat_routes * capacity + slot_of).reshape(tok_count, top_count)
    columns = jnp.arange(ep_count * capacity, dtype=jnp.int32)
    matches = target[:, :, None] == columns[None, None, :]
    placing = jnp.any(matches, axis=1).astype(jnp.bfloat16)
    weighting = jnp.sum(jnp.where(matches, route_weight[:, :, None], 0.0), axis=1)
    outgoing = lax.dot_general(
        placing, normed, (((0,), (0,)), ((), ())), preferred_element_type=jnp.float32
    ).astype(jnp.bfloat16)
    outgoing = outgoing.reshape(ep_count, capacity, model_width)
    gate_up_weight = unpack_rows(gate_up_codes[0], gate_up_scales[0])
    down_weight = unpack_weights(down_codes[0], down_scales[0])
    arrived = lax.all_to_all(outgoing, "ep", split_axis=0, concat_axis=0, tiled=True)
    source_count, item_count, _ = arrived.shape
    flat_rows = arrived.reshape(source_count * item_count, model_width)
    projected = jnp.dot(
        flat_rows, gate_up_weight, preferred_element_type=jnp.float32
    ) + gate_up_bias[0].astype(jnp.float32)
    gate_part = jnp.minimum(projected[:, 0::2], 7.0)
    upward = jnp.clip(projected[:, 1::2], -7.0, 7.0)
    activated = (gate_part * jax.nn.sigmoid(1.702 * gate_part) * (upward + 1.0)).astype(
        jnp.bfloat16
    )
    partial_value = jnp.dot(activated, down_weight, preferred_element_type=jnp.float32)
    partial_value = partial_value.astype(jnp.bfloat16).astype(jnp.float32)
    partial_value = partial_value.reshape(source_count, item_count, model_width)
    summed = lax.psum_scatter(
        partial_value.astype(jnp.bfloat16), "tp", scatter_dimension=2, tiled=True
    ).astype(jnp.float32)
    answered = (summed + down_bias[0].astype(jnp.float32)).astype(jnp.bfloat16)
    came_back = lax.all_to_all(answered, "ep", split_axis=0, concat_axis=0, tiled=True)
    quarter = model_width // tp_count
    own_cols = lax.dynamic_slice_in_dim(hidden, tp_rank * quarter, quarter, 1).astype(jnp.float32)
    gathered = came_back.reshape(ep_count * capacity, quarter).astype(jnp.float32)
    layer_out = own_cols + jnp.dot(weighting, gathered, precision=lax.Precision.HIGHEST)
    return layer_out.astype(jnp.bfloat16)

BF16 = jnp.bfloat16
F32 = jnp.float32
CHUNKS = 2


def word_order(size, lone):
    pos = lax.broadcasted_iota(jnp.int32, (size, size), 1)
    col = lax.broadcasted_iota(jnp.int32, (size, size), 0)
    inner = pos & 63
    source = pos - inner + 8 * (inner & 7) + (inner >> 3)
    if lone:
        last = pos - (size - 32)
        half = size - 32 + 8 * (last & 3) + 2 * (last >> 3) + ((last & 7) >> 2)
        source = jnp.where(last >= 0, half, source)
    return (col == source).astype(F32).astype(BF16)


def matmul(a, b, contract=(1, 0)):
    return lax.dot_general(
        a, b, (((contract[0],), (contract[1],)), ((), ())), preferred_element_type=F32
    )


def column_blocks(total):
    blocks = [(start, 256) for start in range(0, total - total % 256, 256)]
    return blocks + ([(total // 256 * 256, total % 256)] if total % 256 else [])


def magnitude(words, quad):
    return (lax.shift_right_logical(jnp.full_like(words, MAGNITUDES), quad) & 15).astype(F32)


def decode_words(words, scales):
    pieces = []
    for quarter in range(4):
        j = 2 * quarter
        upper = words if j < 4 else lax.shift_right_logical(words, 16)
        pair = jnp.concatenate([upper, lax.shift_right_logical(words, 4 + j // 4 * 16)], axis=0)
        negative = (pair.astype(jnp.int16) & jnp.int16(8 << (4 * (j % 4)))) != 0
        sizes = []
        for i in (j, j + 1):
            moved = jnp.left_shift(words, 2) if i == 0 else lax.shift_right_logical(words, 4 * i - 2)
            sizes.append(magnitude(words, moved & 28))
        scale = scales[quarter]
        pieces.append(
            jnp.concatenate(sizes, axis=0).astype(BF16) * jnp.where(negative, -scale, scale)
        )
    return jnp.concatenate(pieces, axis=0)


def layer_kernel(
    sizes,
    hidden,
    routes,
    route_weights,
    gain,
    gate_codes_in,
    gate_scales_in,
    gate_bias,
    down_codes_in,
    down_scales_in,
    down_bias,
    out,
    gate_codes,
    down_codes,
    half_codes,
    gate_scales,
    down_scales,
    own_part,
    bias_part,
    rows_in,
    gate_weight,
    down_weight,
    activated,
    pair_out,
    pair_in,
    side_out,
    side_in,
    kept,
    step_out,
    step_in,
    load_sem,
    own_send,
    own_recv,
    line_send,
    line_recv,
    cross_send,
    cross_recv,
    pass_send,
    pass_recv,
    pair_send,
    pair_recv,
    side_send,
    side_recv,
    step_send,
    step_recv,
):
    tok, width, n_z, cuts = sizes
    half_rows = tok // 2
    part_rows = half_rows // CHUNKS
    half_cols = width // 2
    ep = lax.axis_index("ep")
    x = lax.axis_index("tp")
    z = ep // 2
    core = ep % 2
    partner = {"ep": 2 * z + 1 - core}
    across = {"tp": 1 - x}
    beside = z + 1 - 2 * (z % 2)
    beyond = (z + 2) % 4
    neighbour = {"ep": 2 * beside + core}
    opposite = {"ep": 2 * beyond + core}

    def copy(src, dst, send, recv, device):
        return pltpu.make_async_remote_copy(
            src_ref=src,
            dst_ref=dst,
            send_sem=send,
            recv_sem=recv,
            device_id=device,
            device_id_type=pl.DeviceIdType.MESH,
        )

    loads = [
        pltpu.make_async_copy(gate_codes_in, gate_codes, load_sem.at[0]),
        pltpu.make_async_copy(down_codes_in, down_codes, load_sem.at[1]),
    ]
    loads[0].start()
    barrier = pltpu.get_barrier_semaphore()
    others = [{"ep": 2 * ((z + d) % n_z) + core} for d in range(1, n_z)]
    for device in [partner, across] + others:
        pl.semaphore_signal(
            barrier, inc=1, device_id=device, device_id_type=pl.DeviceIdType.MESH
        )

    order = word_order(256, False)
    blocks = column_blocks(width)
    gain_row = gain[...].reshape(1, width)
    wide = jnp.concatenate(
        [matmul(hidden[:, c : c + n], order[:n, :n]) for c, n in blocks], axis=1
    )
    gain_row = jnp.concatenate(
        [matmul(gain_row[:, c : c + n], order[:n, :n]) for c, n in blocks], axis=1
    )
    plain = hidden[...].astype(F32)
    mean_square = jnp.mean(plain * plain, axis=-1, keepdims=True)
    normed = (wide * lax.rsqrt(mean_square + 1e-05) * gain_row).astype(BF16)
    number = lax.broadcasted_iota(jnp.int32, (SPARE, tok), 0)
    weight_at = jnp.zeros((SPARE, tok), F32)
    for k in range(routes.shape[0]):
        chosen = routes[k : k + 1, :] == number % (2 * n_z)
        weight_at = weight_at + jnp.where(chosen, route_weights[k : k + 1, :], 0.0)
    high = weight_at.astype(BF16).astype(F32)
    middle = (weight_at - high).astype(BF16).astype(F32)
    low = weight_at - high - middle
    piece = number // (2 * n_z)
    spare = jnp.where(
        piece == 0, high, jnp.where(piece == 1, middle, jnp.where(piece == 2, low, 0.0))
    )
    same = lax.broadcasted_iota(jnp.int32, (tok, tok), 0) == lax.broadcasted_iota(
        jnp.int32, (tok, tok), 1
    )
    spare_lanes = matmul(same.astype(F32).astype(BF16), spare.astype(BF16), (1, 1))
    aligned = width // 128 * 128
    mine = pl.ds(pl.multiple_of(ep * tok, tok), tok)
    rows_in[mine, :aligned] = normed[:, :aligned]
    rows_in[mine, aligned:] = jnp.concatenate(
        [normed[:, aligned:], spare_lanes.astype(BF16)], axis=1
    )

    pl.semaphore_wait(barrier, n_z + 1)

    def part(chip, half, k):
        start = (2 * chip + core) * tok + half * half_rows + k * part_rows
        return rows_in.at[pl.ds(pl.multiple_of(start, part_rows), part_rows)]

    near = 1 - z % 2

    def origin(side, s):
        return (z + n_z + (2 * side - 1) * s) % n_z

    def has(side, s):
        return side * (n_z - 1 - z) + (1 - side) * z >= s

    def goes(side):
        return side * z + (1 - side) * (n_z - 1 - z) >= 1

    def line_copy(side, s, k, chip):
        ref = part(chip, x, k)
        onward = {"ep": 2 * ((z + n_z + 1 - 2 * side) % n_z) + core}
        return copy(ref, ref, line_send.at[side, s, k], line_recv.at[side, s, k], onward)

    def cross_copy(side, s, k):
        ref = part(origin(side, s), x, k)
        return copy(ref, ref, cross_send.at[side, s, k], cross_recv.at[side, s, k], across)

    def pass_copy(side, s, k, i):
        ref = part(origin(side, s), x if i == 0 else 1 - x, k)
        return copy(ref, ref, pass_send.at[side, s, k, i], pass_recv.at[side, s, k, i], partner)

    def when(condition, action):
        pl.when(condition)(action)

    for k in range(CHUNKS):
        for side in range(2):
            when(goes(side), lambda: line_copy(side, 1, k, z).start())

    own_block = rows_in.at[mine]
    own = copy(own_block, own_block, own_send, own_recv, partner)
    own.start()

    def arrive(side, s, k):
        def action():
            line_copy(side, s, k, origin(side, s)).wait_recv()
            if s < n_z - 1:
                when(goes(side), lambda: line_copy(side, s + 1, k, origin(side, s)).start())
            pass_copy(side, s, k, 0).start()

        when(has(side, s), action)

    def cross(side, s, k):
        when(has(side, s), lambda: cross_copy(side, s, k).start())

    def arrive_crossed(side, s, k):
        def action():
            cross_copy(side, s, k).wait_recv()
            pass_copy(side, s, k, 1).start()

        when(has(side, s), action)

    def complete(side, s):
        def action():
            for k in range(CHUNKS):
                for i in range(2):
                    pass_copy(side, s, k, i).wait_recv()

        when(has(side, s), action)

    def drain(side, s):
        def action():
            for k in range(CHUNKS):
                cross_copy(side, s, k).wait_send()
                for i in range(2):
                    pass_copy(side, s, k, i).wait_send()
                if s < n_z - 1:
                    when(
                        goes(side),
                        lambda: line_copy(side, s + 1, k, origin(side, s)).wait_send(),
                    )

        when(has(side, s), action)

    far = 1 - near

    def first_arrives(k):
        arrive(near, 1, k)
        arrive(far, 1, k)
        cross(near, 1, k)

    def later_arrives(s, k):
        arrive(near, s, k)
        arrive(far, s, k)
        cross(near, s, k)
        cross(far, s, k)

    def crossed(s, k):
        arrive_crossed(near, s, k)
        arrive_crossed(far, s, k)

    gate_scales[...] = gate_scales_in[...].astype(F32) * 0.5
    gate_cols = gate_codes.shape[1]
    col_step = 512 if gate_cols % 512 == 0 else 256
    upper = lax.broadcasted_iota(jnp.int32, (16, col_step), 0) % 8 < 4

    def gate_rows(s, carry):
        base = pl.multiple_of(s * 8, 8)
        for col in range(0, gate_cols, col_step):
            words = gate_codes[pl.ds(base, 8), col : col + col_step]
            first, second = (
                jnp.broadcast_to(
                    gate_scales[pl.ds(2 * s + i, 1), col : col + col_step], (16, col_step)
                )
                for i in range(2)
            )
            scale = jnp.where(upper, first, second).astype(BF16)
            gate_weight[pl.ds(pl.multiple_of(s * 64, 64), 64), col : col + col_step] = (
                decode_words(words, [scale] * 4)
            )
        return carry

    gate_steps = gate_codes.shape[0] // 8
    gate_weight[pl.ds(width, SPARE), :] = jnp.zeros((SPARE, gate_cols), BF16)
    scale_rows = down_scales_in.shape[0]
    half_blocks = column_blocks(half_cols)
    tail_size = half_blocks[-1][1]
    tail_order = word_order(tail_size, True)
    for h in range(2):
        for c, n in half_blocks:
            picked = tail_order if n == tail_size else order
            block = down_scales_in[:, h * half_cols + c : h * half_cols + c + n]
            down_scales[h, c : c + n, :scale_rows] = matmul(picked, block, (0, 1)).astype(BF16)
    shown = jnp.where(x == 0, hidden[:, :half_cols], hidden[:, half_cols:])
    for c, n in half_blocks:
        picked = tail_order if n == tail_size else order
        own_part[:, c : c + n] = matmul(shown[:, c : c + n], picked)
        bias_part[:, c : c + n] = matmul(down_bias[:, c : c + n], picked)

    loads[0].wait()
    loads[1].start()
    marks = [0, gate_steps * 20 // 45, gate_steps * 30 // 45, gate_steps * 40 // 45]
    lax.fori_loop(marks[0], marks[1], gate_rows, 0)
    first_arrives(0)
    lax.fori_loop(marks[1], marks[2], gate_rows, 0)
    first_arrives(1)
    for k in range(CHUNKS):
        cross(far, 1, k)
    lax.fori_loop(marks[2], marks[3], gate_rows, 0)
    later_arrives(2, 0)
    lax.fori_loop(marks[3], gate_steps, gate_rows, 0)

    units = down_codes.shape[1]
    words_half = half_cols // 8
    down_steps = words_half // 8
    spread = (
        lax.broadcasted_iota(jnp.int32, (scale_rows, units), 1) // 32
        == lax.broadcasted_iota(jnp.int32, (scale_rows, units), 0)
    ).astype(F32) * 0.5
    spread = spread.astype(BF16)
    loads[1].wait()
    for h in range(2):
        half_codes[h, :words_half] = down_codes[h * words_half : (h + 1) * words_half, :]

    def down_rows(h, g, carry):
        base = pl.multiple_of(g * 128, 128)
        scale_block = down_scales[h, pl.ds(base, 128), :scale_rows]
        for col in range(0, units, 256):
            scale = matmul(scale_block, spread[:, col : col + 256]).astype(BF16)
            for i in range(2):
                words = half_codes[h, pl.ds(pl.multiple_of(g * 16 + 8 * i, 8), 8), col : col + 256]
                start = pl.multiple_of(base + 64 * i, 64)
                down_weight[h, pl.ds(start, 64), col : col + 256] = decode_words(
                    words, [scale[64 * i + 16 * j : 64 * i + 16 * j + 16] for j in range(4)]
                )
        return carry

    place = (lax.broadcasted_iota(jnp.int32, (8, units), 0) >> 2) * 4

    def down_last(h):
        base = down_steps * 64
        four = half_codes[h, down_steps * 8 : words_half, :]
        words = jnp.concatenate([four, four], axis=0)
        scale = matmul(down_scales[h, base : base + 32, :scale_rows], spread)
        pieces = []
        for i in range(4):
            shift = place + 8 * i
            quad = jnp.left_shift(lax.shift_right_logical(words, shift), 2) & 28
            negative = jnp.left_shift(words, 28 - shift) < 0
            part_scale = scale[8 * i : 8 * i + 8]
            pieces.append(magnitude(words, quad) * jnp.where(negative, -part_scale, part_scale))
        down_weight[h, base : base + 32, :] = jnp.concatenate(pieces, axis=0).astype(BF16)

    pair_steps = down_steps // 2
    middle_step = pair_steps // 2
    other_rows = functools.partial(down_rows, 1 - x)
    later_arrives(2, 1)
    lax.fori_loop(0, middle_step, other_rows, 0)
    for k in range(CHUNKS):
        arrive_crossed(near, 1, k)
    own_ahead = pair_steps // 4
    lax.fori_loop(0, own_ahead, functools.partial(down_rows, x), 0)

    picks = (
        lax.broadcasted_iota(jnp.int32, (256, 128), 0)
        == 2 * lax.broadcasted_iota(jnp.int32, (256, 128), 1)
    ).astype(F32).astype(BF16)
    batch_rows = 4 * tok
    group = z // 2
    place_in = z % 2
    starts = [
        pl.multiple_of(group * batch_rows, batch_rows),
        pl.multiple_of((1 - group) * batch_rows, batch_rows),
    ]

    def gate_tile(b, t, tile_cols, steps):
        for step in steps:
            step()
        cols = pl.ds(pl.multiple_of(t * tile_cols, tile_cols), tile_cols)
        projected = jnp.dot(
            rows_in[pl.ds(starts[b], batch_rows), :],
            gate_weight[:, cols],
            preferred_element_type=F32,
        ) + gate_bias[:, cols].astype(F32)
        gate_part = jnp.minimum(projected, 7.0)
        upward = pltpu.roll(jnp.clip(projected, -7.0, 7.0), tile_cols - 1, 1)
        value = (gate_part * jax.nn.sigmoid(1.702 * gate_part) * (upward + 1.0)).astype(BF16)
        for c in range(0, tile_cols, 256):
            at = pl.ds(pl.multiple_of(t * (tile_cols // 2) + c // 2, 128), 128)
            activated[b, :, at] = matmul(value[:, c : c + 256], picks).astype(BF16)

    def pair_copy(b, h, q):
        c, n = cuts[q]
        return copy(
            pair_out.at[b, h, :, :, pl.ds(c, n)],
            pair_in.at[b, h, :, :, pl.ds(c, n)],
            pair_send.at[b, h, q],
            pair_recv.at[b, h, q],
            partner,
        )

    def side_copy(b, i, q):
        c, n = cuts[q]
        return copy(
            side_out.at[b, i, :, pl.ds(c, n)],
            side_in.at[b, i, :, pl.ds(c, n)],
            side_send.at[b, i, q],
            side_recv.at[b, i, q],
            across,
        )

    def step_copy(i, q):
        c, n = cuts[q]
        return copy(
            step_out.at[i, :, pl.ds(c, n)],
            step_in.at[i, :, pl.ds(c, n)],
            step_send.at[i, q],
            step_recv.at[i, q],
            opposite if i == 2 else neighbour,
        )

    tail = lax.broadcasted_iota(jnp.int32, (batch_rows, SPARE), 1)

    def weights_of(b):
        extra = rows_in[pl.ds(starts[b], batch_rows), width:].astype(F32)
        hit = (tail == ep) | (tail == ep + 2 * n_z) | (tail == ep + 4 * n_z)
        return jnp.sum(jnp.where(hit, extra, 0.0), axis=1, keepdims=True)

    parts = range(len(cuts))

    def multiply(b, h, weight, which_parts=parts):
        which = 1 - x if h == 0 else x
        low, high = cuts[which_parts[0]][0], sum(cuts[which_parts[-1]])
        value = matmul(activated[b], down_weight[which, low:high, :], (1, 1))
        if h == 1:
            value = value + bias_part[:, low:high]
        value = value * weight
        for i in range(2):
            first = value[2 * i * tok : (2 * i + 1) * tok]
            second = value[(2 * i + 1) * tok : (2 * i + 2) * tok]
            pair_out[b, h, i, :, low:high] = jnp.where(core == 0, second, first).astype(BF16)
            kept[b, h, i, :, low:high] = jnp.where(core == 0, first, second).astype(BF16)
        for q in which_parts:
            pair_copy(b, h, q).start()

    def fold_pair(b, h, q):
        c, n = cuts[q]
        pair_copy(b, h, q).wait_recv()
        total = kept[b, h, :, :, c : c + n].astype(F32) + pair_in[
            b, h, :, :, c : c + n
        ].astype(F32)
        if h == 0:
            side_out[b, :, :, c : c + n] = total.astype(BF16)
        else:
            kept[b, h, :, :, c : c + n] = total.astype(BF16)

    def folded(b, i, q):
        c, n = cuts[q]
        side_copy(b, i, q).wait_recv()
        return kept[b, 1, i, :, c : c + n].astype(F32) + side_in[b, i, :, c : c + n].astype(F32)

    def fold_side(b, q):
        c, n = cuts[q]
        step_out[b, :, c : c + n] = folded(b, 1 - place_in, q).astype(BF16)
        step_copy(b, q).start()

    def fold_step(q):
        c, n = cuts[q]
        total = folded(1, place_in, q)
        step_copy(1, q).wait_recv()
        total = total + step_in[1, :, c : c + n].astype(F32)
        step_out[2, :, c : c + n] = total.astype(BF16)
        step_copy(2, q).start()

    def fold_own(q):
        c, n = cuts[q]
        total = own_part[:, c : c + n]
        for i in (0, 2):
            step_copy(i, q).wait_recv()
            total = total + step_in[i, :, c : c + n].astype(F32)
        own_part[:, c : c + n] = total + folded(0, place_in, q)

    def write_out(q):
        c, n = cuts[q]
        at = c
        while at < c + n:
            left = half_cols - at
            size = tail_size if left == tail_size else min(256, c + n - at)
            if left > tail_size and left - size < tail_size:
                size = left - tail_size
            picked = tail_order if left == tail_size else order[:size, :size]
            block = own_part[:, at : at + size].astype(BF16)
            out[:, at : at + size] = matmul(block, picked, (1, 1)).astype(BF16)
            at += size


    def decode_steps(which, first, last):
        steps = [functools.partial(down_rows, which, g, 0) for g in range(first, last)]
        return steps + ([functools.partial(down_last, which)] if last == pair_steps else [])

    later_arrives(3, 0)
    own.wait_recv()
    complete(near, 1)
    near_weight = weights_of(0)
    mixed = 512
    tiles = gate_cols // mixed
    own_steps = decode_steps(x, own_ahead, pair_steps)
    early = len(own_steps) // 2
    steps = decode_steps(1 - x, middle_step, pair_steps) + own_steps[:early]
    services = {
        0: [lambda: later_arrives(3, 1)],
        1: [lambda: arrive_crossed(far, 1, 0), lambda: arrive_crossed(far, 1, 1)],
        2: [lambda: crossed(2, 0)],
        3: [lambda: crossed(2, 1), lambda: crossed(3, 0), lambda: crossed(3, 1)],
    }
    for t in range(tiles):
        cut = len(steps) * t // tiles, len(steps) * (t + 1) // tiles
        gate_tile(0, t, mixed, steps[cut[0] : cut[1]])
        for service in services.get(t, []):
            service()
    complete(far, 1)
    for s in range(2, n_z):
        complete(0, s)
        complete(1, s)
    far_weight = weights_of(1)
    gate_tile(1, 0, gate_cols, own_steps[early:])
    multiply(1, 0, far_weight, parts[:2])
    multiply(1, 0, far_weight, parts[2:])

    def send(b, which, q):
        for i in which:
            side_copy(b, i, q).start()

    def sent(b, which, q):
        for i in which:
            side_copy(b, i, q).wait_send()

    theirs, ours = (1 - place_in,), (place_in,)
    for q in parts[:2]:
        fold_pair(1, 0, q)
        send(1, (0, 1), q)
    multiply(1, 1, far_weight)
    for q in parts[2:]:
        fold_pair(1, 0, q)
    multiply(0, 0, near_weight)
    sent(1, (0, 1), 0)
    send(1, (0, 1), 2)
    for q in parts:
        fold_pair(1, 1, q)
    fold_side(1, 0)
    multiply(0, 1, near_weight)
    sent(1, (0, 1), 1)
    send(1, (0, 1), 3)
    for q in parts:
        fold_pair(0, 0, q)
    fold_side(1, 1)
    for q in parts:
        fold_pair(0, 1, q)
    sent(1, (0, 1), 2)
    send(0, theirs, 0)
    send(0, theirs, 1)
    fold_step(0)
    fold_side(1, 2)
    sent(1, (0, 1), 3)
    send(0, theirs, 2)
    send(0, theirs, 3)
    fold_step(1)
    fold_side(1, 3)
    for q in (0, 1):
        sent(0, theirs, q)
        send(0, ours, q)
    fold_step(2)
    for q in (0, 1):
        fold_side(0, q)
    for q in (2, 3):
        sent(0, theirs, q)
        send(0, ours, q)
    fold_step(3)
    for q in (2, 3):
        fold_side(0, q)
    for q in parts:
        fold_own(q)
        write_out(q)

    own.wait_send()
    for side in range(2):

        def sent():
            for k in range(CHUNKS):
                line_copy(side, 1, k, z).wait_send()

        when(goes(side), sent)
        for s in range(1, n_z):
            drain(side, s)
    for q in parts:
        for b in range(2):
            for h in range(2):
                pair_copy(b, h, q).wait_send()
        side_copy(0, place_in, q).wait_send()
        for i in range(3):
            step_copy(i, q).wait_send()


def dense_shards(
    hidden,
    route_experts,
    route_weight,
    norm_gain,
    gate_up_codes,
    gate_up_scales,
    gate_up_bias,
    down_codes,
    down_scales,
    down_bias,
):
    ep_count = lax.axis_size("ep")
    tok, width = hidden.shape
    n_z = ep_count // 2
    half = width // 2
    units = down_codes.shape[1]
    step = -(-half // 512) * 128
    edges = [0] + [step * i - 128 for i in range(1, 4)] + [half]
    cuts = tuple((low, high - low) for low, high in zip(edges[:-1], edges[1:]))
    dma = pltpu.SemaphoreType.DMA
    vmem = pltpu.VMEM
    in_vmem, anywhere = pl.BlockSpec(memory_space=vmem), pl.BlockSpec(memory_space=pl.ANY)
    return pl.pallas_call(
        functools.partial(layer_kernel, (tok, width, n_z, cuts)),
        out_shape=jax.ShapeDtypeStruct((tok, half), BF16),
        in_specs=[in_vmem] * 4 + [anywhere] + [in_vmem] * 2 + [anywhere] + [in_vmem] * 2,
        out_specs=in_vmem,
        scratch_shapes=[
            vmem(gate_up_codes.shape[1:], jnp.int32),
            vmem((down_codes.shape[2], units), jnp.int32),
            vmem((2, -(-half // 64) * 8, units), jnp.int32),
            vmem(gate_up_scales.shape[1:], F32),
            vmem((2, half, 128), BF16),
            vmem((tok, half), F32),
            vmem((1, half), F32),
            vmem((ep_count * tok, width + SPARE), BF16),
            vmem((width + SPARE, gate_up_codes.shape[2]), BF16),
            vmem((2, half, units), BF16),
            vmem((2, ep_count * tok // 2, units), BF16),
            vmem((2, 2, 2, tok, half), BF16),
            vmem((2, 2, 2, tok, half), BF16),
            vmem((2, 2, tok, half), BF16),
            vmem((2, 2, tok, half), BF16),
            vmem((2, 2, 2, tok, half), BF16),
            vmem((3, tok, half), BF16),
            vmem((3, tok, half), BF16),
            dma((2,)),
            dma,
            dma,
            dma((2, n_z, CHUNKS)),
            dma((2, n_z, CHUNKS)),
            dma((2, n_z, CHUNKS)),
            dma((2, n_z, CHUNKS)),
            dma((2, n_z, CHUNKS, 2)),
            dma((2, n_z, CHUNKS, 2)),
            dma((2, 2, 4)),
            dma((2, 2, 4)),
            dma((2, 2, 4)),
            dma((2, 2, 4)),
            dma((3, 4)),
            dma((3, 4)),
        ],
        compiler_params=pltpu.CompilerParams(
            collective_id=0, has_side_effects=True, vmem_limit_bytes=63 * 1024 * 1024
        ),
    )(
        hidden,
        route_experts.T,
        route_weight.T,
        norm_gain,
        gate_up_codes[0],
        gate_up_scales[0],
        gate_up_bias,
        down_codes[0].T,
        down_scales[0],
        down_bias,
    )


def solution(mesh):
    def layer(*arrays):
        tok, top = arrays[1].shape
        ep_count, tp_count = lax.axis_size("ep"), lax.axis_size("tp")
        dense = 2 * top >= ep_count and tp_count == 2 and ep_count == 8 and tok == 64
        return (dense_shards if dense else shards)(*arrays)

    placed = (
        P(("groups", "ep"), None),
        P(("groups", "ep"), None),
        P(("groups", "ep"), None),
        P(),
        P("ep", None, "tp"),
        P("ep", None, "tp"),
        P("ep", "tp"),
        P("ep", "tp", None),
        P("ep", "tp", None),
        P("ep", "tp"),
    )
    return jax.shard_map(
        layer, mesh=mesh, in_specs=placed, out_specs=P(("groups", "ep"), "tp"), check_vma=False
    )
```

```python
import functools

import jax
import jax.numpy as jnp
from jax import lax
from jax.experimental import pallas as pl
from jax.experimental.pallas import tpu as pltpu
from jax.sharding import PartitionSpec as P

MAGNITUDES = 0xC8643210 - (1 << 32)
SPARE = 64


def decode_nibble(nibble):
    magnit = nibble & 7
    exponent = jnp.maximum(jnp.right_shift(magnit, 1) - 1, 0)
    doubled = jnp.where(magnit < 2, magnit, jnp.left_shift(2 + (magnit & 1), exponent))
    signed_val = doubled.astype(jnp.float32) * 0.5
    return jnp.where(nibble >= 8, -signed_val, signed_val)


def unpack_weights(packed, scaling):
    row_count = packed.shape[0]
    shifts = jnp.arange(8, dtype=jnp.int32) * 4
    nibble = jnp.right_shift(packed[:, :, None], shifts[None, None, :]) & 15
    nibble = nibble.reshape(row_count, packed.shape[1] * 8)
    signed_val = decode_nibble(nibble)
    signed_val = (
        signed_val.reshape(row_count // 32, 32, -1) * scaling.astype(jnp.float32)[:, None, :]
    )
    return signed_val.reshape(row_count, -1).astype(jnp.bfloat16)


def unpack_rows(packed, scaling):
    row_count = packed.shape[0] * 8
    shifts = jnp.arange(8, dtype=jnp.int32) * 4
    nibble = jnp.right_shift(packed[:, None, :], shifts[None, :, None]) & 15
    nibble = nibble.reshape(row_count, packed.shape[1])
    signed_val = decode_nibble(nibble)
    signed_val = (
        signed_val.reshape(row_count // 32, 32, -1) * scaling.astype(jnp.float32)[:, None, :]
    )
    return signed_val.reshape(row_count, -1).astype(jnp.bfloat16)


def rms_normed(hidden, norm_gain):
    widened = hidden.astype(jnp.float32)
    mean_square = jnp.mean(widened * widened, axis=-1, keepdims=True)
    scaled = widened * lax.rsqrt(mean_square + 1e-05) * norm_gain.astype(jnp.float32)
    return scaled.astype(jnp.bfloat16)


def shards(
    hidden,
    route_experts,
    route_weight,
    norm_gain,
    gate_up_codes,
    gate_up_scales,
    gate_up_bias,
    down_codes,
    down_scales,
    down_bias,
):
    ep_count = lax.axis_size("ep")
    tp_count = lax.axis_size("tp")
    tp_rank = lax.axis_index("tp")
    tok_count, model_width = hidden.shape
    top_count = route_experts.shape[1]
    capacity = min(tok_count, max(tp_count, 2 * tok_count * top_count // ep_count))
    normed = rms_normed(hidden, norm_gain)
    flat_routes = route_experts.reshape(-1)
    onehot = (flat_routes[:, None] == jnp.arange(ep_count, dtype=jnp.int32)[None, :]).astype(
        jnp.int32
    )
    before = jnp.cumsum(onehot, axis=0) - onehot
    slot_of = jnp.sum(before * onehot, axis=1)
    target = (flat_routes * capacity + slot_of).reshape(tok_count, top_count)
    columns = jnp.arange(ep_count * capacity, dtype=jnp.int32)
    matches = target[:, :, None] == columns[None, None, :]
    placing = jnp.any(matches, axis=1).astype(jnp.bfloat16)
    weighting = jnp.sum(jnp.where(matches, route_weight[:, :, None], 0.0), axis=1)
    outgoing = lax.dot_general(
        placing, normed, (((0,), (0,)), ((), ())), preferred_element_type=jnp.float32
    ).astype(jnp.bfloat16)
    outgoing = outgoing.reshape(ep_count, capacity, model_width)
    gate_up_weight = unpack_rows(gate_up_codes[0], gate_up_scales[0])
    down_weight = unpack_weights(down_codes[0], down_scales[0])
    arrived = lax.all_to_all(outgoing, "ep", split_axis=0, concat_axis=0, tiled=True)
    source_count, item_count, _ = arrived.shape
    flat_rows = arrived.reshape(source_count * item_count, model_width)
    projected = jnp.dot(
        flat_rows, gate_up_weight, preferred_element_type=jnp.float32
    ) + gate_up_bias[0].astype(jnp.float32)
    gate_part = jnp.minimum(projected[:, 0::2], 7.0)
    upward = jnp.clip(projected[:, 1::2], -7.0, 7.0)
    activated = (gate_part * jax.nn.sigmoid(1.702 * gate_part) * (upward + 1.0)).astype(
        jnp.bfloat16
    )
    partial_value = jnp.dot(activated, down_weight, preferred_element_type=jnp.float32)
    partial_value = partial_value.astype(jnp.bfloat16).astype(jnp.float32)
    partial_value = partial_value.reshape(source_count, item_count, model_width)
    summed = lax.psum_scatter(
        partial_value.astype(jnp.bfloat16), "tp", scatter_dimension=2, tiled=True
    ).astype(jnp.float32)
    answered = (summed + down_bias[0].astype(jnp.float32)).astype(jnp.bfloat16)
    came_back = lax.all_to_all(answered, "ep", split_axis=0, concat_axis=0, tiled=True)
    quarter = model_width // tp_count
    own_cols = lax.dynamic_slice_in_dim(hidden, tp_rank * quarter, quarter, 1).astype(jnp.float32)
    gathered = came_back.reshape(ep_count * capacity, quarter).astype(jnp.float32)
    layer_out = own_cols + jnp.dot(weighting, gathered, precision=lax.Precision.HIGHEST)
    return layer_out.astype(jnp.bfloat16)

BF16 = jnp.bfloat16
F32 = jnp.float32
CHUNKS = 2


def word_order(size, lone):
    pos = lax.broadcasted_iota(jnp.int32, (size, size), 1)
    col = lax.broadcasted_iota(jnp.int32, (size, size), 0)
    inner = pos & 63
    source = pos - inner + 8 * (inner & 7) + (inner >> 3)
    if lone:
        last = pos - (size - 32)
        half = size - 32 + 8 * (last & 3) + 2 * (last >> 3) + ((last & 7) >> 2)
        source = jnp.where(last >= 0, half, source)
    return (col == source).astype(F32).astype(BF16)


def matmul(a, b, contract=(1, 0)):
    return lax.dot_general(
        a, b, (((contract[0],), (contract[1],)), ((), ())), preferred_element_type=F32
    )


def column_blocks(total):
    blocks = [(start, 256) for start in range(0, total - total % 256, 256)]
    return blocks + ([(total // 256 * 256, total % 256)] if total % 256 else [])


def magnitude(words, quad):
    return (lax.shift_right_logical(jnp.full_like(words, MAGNITUDES), quad) & 15).astype(F32)


def decode_words(words, scales):
    pieces = []
    for quarter in range(4):
        j = 2 * quarter
        upper = words if j < 4 else lax.shift_right_logical(words, 16)
        pair = jnp.concatenate([upper, lax.shift_right_logical(words, 4 + j // 4 * 16)], axis=0)
        negative = (pair.astype(jnp.int16) & jnp.int16(8 << (4 * (j % 4)))) != 0
        sizes = []
        for i in (j, j + 1):
            moved = jnp.left_shift(words, 2) if i == 0 else lax.shift_right_logical(words, 4 * i - 2)
            sizes.append(magnitude(words, moved & 28))
        scale = scales[quarter]
        pieces.append(
            jnp.concatenate(sizes, axis=0).astype(BF16) * jnp.where(negative, -scale, scale)
        )
    return jnp.concatenate(pieces, axis=0)


def layer_kernel(
    sizes,
    hidden,
    routes,
    route_weights,
    gain,
    gate_codes_in,
    gate_scales_in,
    gate_bias,
    down_codes_in,
    down_scales_in,
    down_bias,
    out,
    gate_codes,
    down_codes,
    half_codes,
    gate_scales,
    down_scales,
    own_part,
    bias_part,
    rows_in,
    gate_weight,
    down_weight,
    activated,
    pair_out,
    pair_in,
    side_out,
    side_in,
    kept,
    step_out,
    step_in,
    load_sem,
    own_send,
    own_recv,
    line_send,
    line_recv,
    cross_send,
    cross_recv,
    pass_send,
    pass_recv,
    pair_send,
    pair_recv,
    side_send,
    side_recv,
    step_send,
    step_recv,
):
    tok, width, n_z, cuts = sizes
    half_rows = tok // 2
    part_rows = half_rows // CHUNKS
    half_cols = width // 2
    ep = lax.axis_index("ep")
    x = lax.axis_index("tp")
    z = ep // 2
    core = ep % 2
    partner = {"ep": 2 * z + 1 - core}
    across = {"tp": 1 - x}
    beside = z + 1 - 2 * (z % 2)
    beyond = (z + 2) % 4
    neighbour = {"ep": 2 * beside + core}
    opposite = {"ep": 2 * beyond + core}

    def copy(src, dst, send, recv, device):
        return pltpu.make_async_remote_copy(
            src_ref=src,
            dst_ref=dst,
            send_sem=send,
            recv_sem=recv,
            device_id=device,
            device_id_type=pl.DeviceIdType.MESH,
        )

    loads = [
        pltpu.make_async_copy(gate_codes_in, gate_codes, load_sem.at[0]),
        pltpu.make_async_copy(down_codes_in, down_codes, load_sem.at[1]),
    ]
    loads[0].start()
    barrier = pltpu.get_barrier_semaphore()
    others = [{"ep": 2 * ((z + d) % n_z) + core} for d in range(1, n_z)]
    for device in [partner, across] + others:
        pl.semaphore_signal(
            barrier, inc=1, device_id=device, device_id_type=pl.DeviceIdType.MESH
        )

    order = word_order(256, False)
    blocks = column_blocks(width)
    gain_row = gain[...].reshape(1, width)
    wide = jnp.concatenate(
        [matmul(hidden[:, c : c + n], order[:n, :n]) for c, n in blocks], axis=1
    )
    gain_row = jnp.concatenate(
        [matmul(gain_row[:, c : c + n], order[:n, :n]) for c, n in blocks], axis=1
    )
    plain = hidden[...].astype(F32)
    mean_square = jnp.mean(plain * plain, axis=-1, keepdims=True)
    normed = (wide * lax.rsqrt(mean_square + 1e-05) * gain_row).astype(BF16)
    number = lax.broadcasted_iota(jnp.int32, (SPARE, tok), 0)
    weight_at = jnp.zeros((SPARE, tok), F32)
    for k in range(routes.shape[0]):
        chosen = routes[k : k + 1, :] == number % (2 * n_z)
        weight_at = weight_at + jnp.where(chosen, route_weights[k : k + 1, :], 0.0)
    high = weight_at.astype(BF16).astype(F32)
    middle = (weight_at - high).astype(BF16).astype(F32)
    low = weight_at - high - middle
    piece = number // (2 * n_z)
    spare = jnp.where(
        piece == 0, high, jnp.where(piece == 1, middle, jnp.where(piece == 2, low, 0.0))
    )
    same = lax.broadcasted_iota(jnp.int32, (tok, tok), 0) == lax.broadcasted_iota(
        jnp.int32, (tok, tok), 1
    )
    spare_lanes = matmul(same.astype(F32).astype(BF16), spare.astype(BF16), (1, 1))
    aligned = width // 128 * 128
    mine = pl.ds(pl.multiple_of(ep * tok, tok), tok)
    rows_in[mine, :aligned] = normed[:, :aligned]
    rows_in[mine, aligned:] = jnp.concatenate(
        [normed[:, aligned:], spare_lanes.astype(BF16)], axis=1
    )

    pl.semaphore_wait(barrier, n_z + 1)

    def part(chip, half, k):
        start = (2 * chip + core) * tok + half * half_rows + k * part_rows
        return rows_in.at[pl.ds(pl.multiple_of(start, part_rows), part_rows)]

    near = 1 - z % 2

    def origin(side, s):
        return (z + n_z + (2 * side - 1) * s) % n_z

    def has(side, s):
        return side * (n_z - 1 - z) + (1 - side) * z >= s

    def goes(side):
        return side * z + (1 - side) * (n_z - 1 - z) >= 1

    def line_copy(side, s, k, chip):
        ref = part(chip, x, k)
        onward = {"ep": 2 * ((z + n_z + 1 - 2 * side) % n_z) + core}
        return copy(ref, ref, line_send.at[side, s, k], line_recv.at[side, s, k], onward)

    def cross_copy(side, s, k):
        ref = part(origin(side, s), x, k)
        return copy(ref, ref, cross_send.at[side, s, k], cross_recv.at[side, s, k], across)

    def pass_copy(side, s, k, i):
        ref = part(origin(side, s), x if i == 0 else 1 - x, k)
        return copy(ref, ref, pass_send.at[side, s, k, i], pass_recv.at[side, s, k, i], partner)

    def when(condition, action):
        pl.when(condition)(action)

    for k in range(CHUNKS):
        for side in range(2):
            when(goes(side), lambda: line_copy(side, 1, k, z).start())

    own_block = rows_in.at[mine]
    own = copy(own_block, own_block, own_send, own_recv, partner)
    own.start()

    def arrive(side, s, k):
        def action():
            line_copy(side, s, k, origin(side, s)).wait_recv()
            if s < n_z - 1:
                when(goes(side), lambda: line_copy(side, s + 1, k, origin(side, s)).start())
            pass_copy(side, s, k, 0).start()

        when(has(side, s), action)

    def cross(side, s, k):
        when(has(side, s), lambda: cross_copy(side, s, k).start())

    def arrive_crossed(side, s, k):
        def action():
            cross_copy(side, s, k).wait_recv()
            pass_copy(side, s, k, 1).start()

        when(has(side, s), action)

    def complete(side, s):
        def action():
            for k in range(CHUNKS):
                for i in range(2):
                    pass_copy(side, s, k, i).wait_recv()

        when(has(side, s), action)

    def drain(side, s):
        def action():
            for k in range(CHUNKS):
                cross_copy(side, s, k).wait_send()
                for i in range(2):
                    pass_copy(side, s, k, i).wait_send()
                if s < n_z - 1:
                    when(
                        goes(side),
                        lambda: line_copy(side, s + 1, k, origin(side, s)).wait_send(),
                    )

        when(has(side, s), action)

    far = 1 - near

    def first_arrives(k):
        arrive(near, 1, k)
        arrive(far, 1, k)
        cross(near, 1, k)

    def later_arrives(s, k):
        arrive(near, s, k)
        arrive(far, s, k)
        cross(near, s, k)
        cross(far, s, k)

    def crossed(s, k):
        arrive_crossed(near, s, k)
        arrive_crossed(far, s, k)

    gate_scales[...] = gate_scales_in[...].astype(F32) * 0.5
    gate_cols = gate_codes.shape[1]
    col_step = 512 if gate_cols % 512 == 0 else 256
    upper = lax.broadcasted_iota(jnp.int32, (16, col_step), 0) % 8 < 4

    def gate_rows(s, carry):
        base = pl.multiple_of(s * 8, 8)
        for col in range(0, gate_cols, col_step):
            words = gate_codes[pl.ds(base, 8), col : col + col_step]
            first, second = (
                jnp.broadcast_to(
                    gate_scales[pl.ds(2 * s + i, 1), col : col + col_step], (16, col_step)
                )
                for i in range(2)
            )
            scale = jnp.where(upper, first, second).astype(BF16)
            gate_weight[pl.ds(pl.multiple_of(s * 64, 64), 64), col : col + col_step] = (
                decode_words(words, [scale] * 4)
            )
        return carry

    gate_steps = gate_codes.shape[0] // 8
    gate_weight[pl.ds(width, SPARE), :] = jnp.zeros((SPARE, gate_cols), BF16)
    scale_rows = down_scales_in.shape[0]
    half_blocks = column_blocks(half_cols)
    tail_size = half_blocks[-1][1]
    tail_order = word_order(tail_size, True)
    for h in range(2):
        for c, n in half_blocks:
            picked = tail_order if n == tail_size else order
            block = down_scales_in[:, h * half_cols + c : h * half_cols + c + n]
            down_scales[h, c : c + n, :scale_rows] = matmul(picked, block, (0, 1)).astype(BF16)
    shown = jnp.where(x == 0, hidden[:, :half_cols], hidden[:, half_cols:])
    for c, n in half_blocks:
        picked = tail_order if n == tail_size else order
        own_part[:, c : c + n] = matmul(shown[:, c : c + n], picked)
        bias_part[:, c : c + n] = matmul(down_bias[:, c : c + n], picked)

    loads[0].wait()
    loads[1].start()
    marks = [0, gate_steps * 20 // 45, gate_steps * 30 // 45, gate_steps * 40 // 45]
    lax.fori_loop(marks[0], marks[1], gate_rows, 0)
    first_arrives(0)
    lax.fori_loop(marks[1], marks[2], gate_rows, 0)
    first_arrives(1)
    for k in range(CHUNKS):
        cross(far, 1, k)
    lax.fori_loop(marks[2], marks[3], gate_rows, 0)
    later_arrives(2, 0)
    lax.fori_loop(marks[3], gate_steps, gate_rows, 0)

    units = down_codes.shape[1]
    words_half = half_cols // 8
    down_steps = words_half // 8
    spread = (
        lax.broadcasted_iota(jnp.int32, (scale_rows, units), 1) // 32
        == lax.broadcasted_iota(jnp.int32, (scale_rows, units), 0)
    ).astype(F32) * 0.5
    spread = spread.astype(BF16)
    loads[1].wait()
    for h in range(2):
        half_codes[h, :words_half] = down_codes[h * words_half : (h + 1) * words_half, :]

    def down_rows(h, g, carry):
        base = pl.multiple_of(g * 128, 128)
        scale_block = down_scales[h, pl.ds(base, 128), :scale_rows]
        for col in range(0, units, 256):
            scale = matmul(scale_block, spread[:, col : col + 256]).astype(BF16)
            for i in range(2):
                words = half_codes[h, pl.ds(pl.multiple_of(g * 16 + 8 * i, 8), 8), col : col + 256]
                start = pl.multiple_of(base + 64 * i, 64)
                down_weight[h, pl.ds(start, 64), col : col + 256] = decode_words(
                    words, [scale[64 * i + 16 * j : 64 * i + 16 * j + 16] for j in range(4)]
                )
        return carry

    place = (lax.broadcasted_iota(jnp.int32, (8, units), 0) >> 2) * 4

    def down_last(h):
        base = down_steps * 64
        four = half_codes[h, down_steps * 8 : words_half, :]
        words = jnp.concatenate([four, four], axis=0)
        scale = matmul(down_scales[h, base : base + 32, :scale_rows], spread)
        pieces = []
        for i in range(4):
            shift = place + 8 * i
            quad = jnp.left_shift(lax.shift_right_logical(words, shift), 2) & 28
            negative = jnp.left_shift(words, 28 - shift) < 0
            part_scale = scale[8 * i : 8 * i + 8]
            pieces.append(magnitude(words, quad) * jnp.where(negative, -part_scale, part_scale))
        down_weight[h, base : base + 32, :] = jnp.concatenate(pieces, axis=0).astype(BF16)

    pair_steps = down_steps // 2
    middle_step = pair_steps // 2
    other_rows = functools.partial(down_rows, 1 - x)
    later_arrives(2, 1)
    lax.fori_loop(0, middle_step, other_rows, 0)
    for k in range(CHUNKS):
        arrive_crossed(near, 1, k)
    own_ahead = pair_steps // 4
    lax.fori_loop(0, own_ahead, functools.partial(down_rows, x), 0)

    picks = (
        lax.broadcasted_iota(jnp.int32, (256, 128), 0)
        == 2 * lax.broadcasted_iota(jnp.int32, (256, 128), 1)
    ).astype(F32).astype(BF16)
    batch_rows = 4 * tok
    group = z // 2
    place_in = z % 2
    starts = [
        pl.multiple_of(group * batch_rows, batch_rows),
        pl.multiple_of((1 - group) * batch_rows, batch_rows),
    ]

    def gate_tile(b, t, tile_cols, steps):
        for step in steps:
            step()
        cols = pl.ds(pl.multiple_of(t * tile_cols, tile_cols), tile_cols)
        projected = jnp.dot(
            rows_in[pl.ds(starts[b], batch_rows), :],
            gate_weight[:, cols],
            preferred_element_type=F32,
        ) + gate_bias[:, cols].astype(F32)
        gate_part = jnp.minimum(projected, 7.0)
        upward = pltpu.roll(jnp.clip(projected, -7.0, 7.0), tile_cols - 1, 1)
        value = (gate_part * jax.nn.sigmoid(1.702 * gate_part) * (upward + 1.0)).astype(BF16)
        for c in range(0, tile_cols, 256):
            at = pl.ds(pl.multiple_of(t * (tile_cols // 2) + c // 2, 128), 128)
            activated[b, :, at] = matmul(value[:, c : c + 256], picks).astype(BF16)

    def pair_copy(b, h, q):
        c, n = cuts[q]
        return copy(
            pair_out.at[b, h, :, :, pl.ds(c, n)],
            pair_in.at[b, h, :, :, pl.ds(c, n)],
            pair_send.at[b, h, q],
            pair_recv.at[b, h, q],
            partner,
        )

    def side_copy(b, i, q):
        c, n = cuts[q]
        return copy(
            side_out.at[b, i, :, pl.ds(c, n)],
            side_in.at[b, i, :, pl.ds(c, n)],
            side_send.at[b, i, q],
            side_recv.at[b, i, q],
            across,
        )

    def step_copy(i, q):
        c, n = cuts[q]
        return copy(
            step_out.at[i, :, pl.ds(c, n)],
            step_in.at[i, :, pl.ds(c, n)],
            step_send.at[i, q],
            step_recv.at[i, q],
            opposite if i == 2 else neighbour,
        )

    tail = lax.broadcasted_iota(jnp.int32, (batch_rows, SPARE), 1)

    def weights_of(b):
        extra = rows_in[pl.ds(starts[b], batch_rows), width:].astype(F32)
        hit = (tail == ep) | (tail == ep + 2 * n_z) | (tail == ep + 4 * n_z)
        return jnp.sum(jnp.where(hit, extra, 0.0), axis=1, keepdims=True)

    parts = range(len(cuts))

    def multiply(b, h, weight, which_parts=parts):
        which = 1 - x if h == 0 else x
        low, high = cuts[which_parts[0]][0], sum(cuts[which_parts[-1]])
        value = matmul(activated[b], down_weight[which, low:high, :], (1, 1))
        if h == 1:
            value = value + bias_part[:, low:high]
        value = value * weight
        for i in range(2):
            first = value[2 * i * tok : (2 * i + 1) * tok]
            second = value[(2 * i + 1) * tok : (2 * i + 2) * tok]
            pair_out[b, h, i, :, low:high] = jnp.where(core == 0, second, first).astype(BF16)
            kept[b, h, i, :, low:high] = jnp.where(core == 0, first, second).astype(BF16)
        for q in which_parts:
            pair_copy(b, h, q).start()

    def fold_pair(b, h, q):
        c, n = cuts[q]
        pair_copy(b, h, q).wait_recv()
        total = kept[b, h, :, :, c : c + n].astype(F32) + pair_in[
            b, h, :, :, c : c + n
        ].astype(F32)
        if h == 0:
            side_out[b, :, :, c : c + n] = total.astype(BF16)
        else:
            kept[b, h, :, :, c : c + n] = total.astype(BF16)

    def folded(b, i, q):
        c, n = cuts[q]
        side_copy(b, i, q).wait_recv()
        return kept[b, 1, i, :, c : c + n].astype(F32) + side_in[b, i, :, c : c + n].astype(F32)

    def fold_side(b, q):
        c, n = cuts[q]
        step_out[b, :, c : c + n] = folded(b, 1 - place_in, q).astype(BF16)
        step_copy(b, q).start()

    def fold_step(q):
        c, n = cuts[q]
        total = folded(1, place_in, q)
        step_copy(1, q).wait_recv()
        total = total + step_in[1, :, c : c + n].astype(F32)
        step_out[2, :, c : c + n] = total.astype(BF16)
        step_copy(2, q).start()

    def fold_own(q):
        c, n = cuts[q]
        total = own_part[:, c : c + n]
        for i in (0, 2):
            step_copy(i, q).wait_recv()
            total = total + step_in[i, :, c : c + n].astype(F32)
        own_part[:, c : c + n] = total + folded(0, place_in, q)

    def write_out(q):
        c, n = cuts[q]
        at = c
        while at < c + n:
            left = half_cols - at
            size = tail_size if left == tail_size else min(256, c + n - at)
            if left > tail_size and left - size < tail_size:
                size = left - tail_size
            picked = tail_order if left == tail_size else order[:size, :size]
            block = own_part[:, at : at + size].astype(BF16)
            out[:, at : at + size] = matmul(block, picked, (1, 1)).astype(BF16)
            at += size


    def decode_steps(which, first, last):
        steps = [functools.partial(down_rows, which, g, 0) for g in range(first, last)]
        return steps + ([functools.partial(down_last, which)] if last == pair_steps else [])

    later_arrives(3, 0)
    own.wait_recv()
    complete(near, 1)
    near_weight = weights_of(0)
    mixed = 512
    tiles = gate_cols // mixed
    own_steps = decode_steps(x, own_ahead, pair_steps)
    early = len(own_steps) // 2
    steps = decode_steps(1 - x, middle_step, pair_steps) + own_steps[:early]
    services = {
        0: [lambda: later_arrives(3, 1)],
        1: [lambda: arrive_crossed(far, 1, 0), lambda: arrive_crossed(far, 1, 1)],
        2: [lambda: crossed(2, 0)],
        3: [lambda: crossed(2, 1), lambda: crossed(3, 0), lambda: crossed(3, 1)],
    }
    for t in range(tiles - 1):
        cut = len(steps) * t // (tiles - 1), len(steps) * (t + 1) // (tiles - 1)
        gate_tile(0, t, mixed, steps[cut[0] : cut[1]])
        for service in services.get(t, []):
            service()
    for step in own_steps[early:]:
        step()
    complete(far, 1)
    for s in range(2, n_z):
        complete(0, s)
        complete(1, s)
    far_weight = weights_of(1)
    gate_tile(1, 0, gate_cols, [])
    multiply(1, 0, far_weight, parts[:2])
    multiply(1, 0, far_weight, parts[2:])

    def send(b, which, q):
        for i in which:
            side_copy(b, i, q).start()

    def sent(b, which, q):
        for i in which:
            side_copy(b, i, q).wait_send()

    theirs, ours = (1 - place_in,), (place_in,)
    for q in parts[:2]:
        fold_pair(1, 0, q)
        send(1, (0, 1), q)
    multiply(1, 1, far_weight)
    for q in parts[2:]:
        fold_pair(1, 0, q)
    gate_tile(0, tiles - 1, mixed, [])
    sent(1, (0, 1), 0)
    send(1, (0, 1), 2)
    for q in parts:
        fold_pair(1, 1, q)
    fold_side(1, 0)
    multiply(0, 0, near_weight)
    multiply(0, 1, near_weight)
    sent(1, (0, 1), 1)
    send(1, (0, 1), 3)
    for q in parts:
        fold_pair(0, 0, q)
    fold_side(1, 1)
    for q in parts:
        fold_pair(0, 1, q)
    sent(1, (0, 1), 2)
    send(0, theirs, 0)
    send(0, theirs, 1)
    fold_step(0)
    fold_side(1, 2)
    sent(1, (0, 1), 3)
    send(0, theirs, 2)
    send(0, theirs, 3)
    fold_step(1)
    fold_side(1, 3)
    for q in (0, 1):
        sent(0, theirs, q)
        send(0, ours, q)
    fold_step(2)
    for q in (0, 1):
        fold_side(0, q)
    for q in (2, 3):
        sent(0, theirs, q)
        send(0, ours, q)
    fold_step(3)
    for q in (2, 3):
        fold_side(0, q)
    for q in parts:
        fold_own(q)
        write_out(q)

    own.wait_send()
    for side in range(2):

        def sent():
            for k in range(CHUNKS):
                line_copy(side, 1, k, z).wait_send()

        when(goes(side), sent)
        for s in range(1, n_z):
            drain(side, s)
    for q in parts:
        for b in range(2):
            for h in range(2):
                pair_copy(b, h, q).wait_send()
        side_copy(0, place_in, q).wait_send()
        for i in range(3):
            step_copy(i, q).wait_send()


def dense_shards(
    hidden,
    route_experts,
    route_weight,
    norm_gain,
    gate_up_codes,
    gate_up_scales,
    gate_up_bias,
    down_codes,
    down_scales,
    down_bias,
):
    ep_count = lax.axis_size("ep")
    tok, width = hidden.shape
    n_z = ep_count // 2
    half = width // 2
    units = down_codes.shape[1]
    step = -(-half // 512) * 128
    edges = [0] + [step * i - 128 for i in range(1, 4)] + [half]
    cuts = tuple((low, high - low) for low, high in zip(edges[:-1], edges[1:]))
    dma = pltpu.SemaphoreType.DMA
    vmem = pltpu.VMEM
    in_vmem, anywhere = pl.BlockSpec(memory_space=vmem), pl.BlockSpec(memory_space=pl.ANY)
    return pl.pallas_call(
        functools.partial(layer_kernel, (tok, width, n_z, cuts)),
        out_shape=jax.ShapeDtypeStruct((tok, half), BF16),
        in_specs=[in_vmem] * 4 + [anywhere] + [in_vmem] * 2 + [anywhere] + [in_vmem] * 2,
        out_specs=in_vmem,
        scratch_shapes=[
            vmem(gate_up_codes.shape[1:], jnp.int32),
            vmem((down_codes.shape[2], units), jnp.int32),
            vmem((2, -(-half // 64) * 8, units), jnp.int32),
            vmem(gate_up_scales.shape[1:], F32),
            vmem((2, half, 128), BF16),
            vmem((tok, half), F32),
            vmem((1, half), F32),
            vmem((ep_count * tok, width + SPARE), BF16),
            vmem((width + SPARE, gate_up_codes.shape[2]), BF16),
            vmem((2, half, units), BF16),
            vmem((2, ep_count * tok // 2, units), BF16),
            vmem((2, 2, 2, tok, half), BF16),
            vmem((2, 2, 2, tok, half), BF16),
            vmem((2, 2, tok, half), BF16),
            vmem((2, 2, tok, half), BF16),
            vmem((2, 2, 2, tok, half), BF16),
            vmem((3, tok, half), BF16),
            vmem((3, tok, half), BF16),
            dma((2,)),
            dma,
            dma,
            dma((2, n_z, CHUNKS)),
            dma((2, n_z, CHUNKS)),
            dma((2, n_z, CHUNKS)),
            dma((2, n_z, CHUNKS)),
            dma((2, n_z, CHUNKS, 2)),
            dma((2, n_z, CHUNKS, 2)),
            dma((2, 2, 4)),
            dma((2, 2, 4)),
            dma((2, 2, 4)),
            dma((2, 2, 4)),
            dma((3, 4)),
            dma((3, 4)),
        ],
        compiler_params=pltpu.CompilerParams(
            collective_id=0, has_side_effects=True, vmem_limit_bytes=63 * 1024 * 1024
        ),
    )(
        hidden,
        route_experts.T,
        route_weight.T,
        norm_gain,
        gate_up_codes[0],
        gate_up_scales[0],
        gate_up_bias,
        down_codes[0].T,
        down_scales[0],
        down_bias,
    )


def solution(mesh):
    def layer(*arrays):
        tok, top = arrays[1].shape
        ep_count, tp_count = lax.axis_size("ep"), lax.axis_size("tp")
        dense = 2 * top >= ep_count and tp_count == 2 and ep_count == 8 and tok == 64
        return (dense_shards if dense else shards)(*arrays)

    placed = (
        P(("groups", "ep"), None),
        P(("groups", "ep"), None),
        P(("groups", "ep"), None),
        P(),
        P("ep", None, "tp"),
        P("ep", None, "tp"),
        P("ep", "tp"),
        P("ep", "tp", None),
        P("ep", "tp", None),
        P("ep", "tp"),
    )
    return jax.shard_map(
        layer, mesh=mesh, in_specs=placed, out_specs=P(("groups", "ep"), "tp"), check_vma=False
    )
```
